256 devices in a mesh: section: 8 (over y, x_lo), dev: 32 (over x_hi, z, core).
Axes of the slice: x: 4 (x_hi: 2, x_lo: 2; x = x_hi * 2 + x_lo), y: 4, z: 8, core: 2. Of those that a mesh axis runs over, the one named last changes fastest.
Arguments:
- late_sent: bfloat16 [8, 3136, 1024], P('section', 'dev'), may hold values from -5 to 5
- entry_rows: bfloat16 [3136, 1024], P('dev'), may hold values from -5 to 5
- gain_first: float32 [8, 1024], P('section'), may hold values from 0.1 to 1.9
- shift_first: float32 [8, 1024], P('section'), may hold values from -3 to 3
- expand_late: bfloat16 [8, 1024, 4096], P('section', None, 'dev'), may hold values from -0.1875 to 0.1875
- gain_inner: float32 [8, 4096], P('section', 'dev'), may hold values from 0.1 to 1.9
- shift_inner: float32 [8, 4096], P('section', 'dev'), may hold values from -3 to 3
- reduce_late: bfloat16 [8, 4096, 1024], P('section', 'dev'), may hold values from -0.09375 to 0.09375
- early_saved: bfloat16 [8, 50176, 256], P('section', 'dev'), may hold values from -6 to 6
- upstream_grad: bfloat16 [8, 50176, 256], P('section', 'dev'), may hold values from -6 to 6
- exit_grad: bfloat16 [50176, 256], P('dev'), may hold values from -6 to 6
- expand_early: bfloat16 [8, 256, 1024], P('section'), may hold values from -0.375 to 0.375
- reduce_early: bfloat16 [8, 1024, 256], P('section'), may hold values from -0.1875 to 0.1875
Outputs:
- late_out: bfloat16 [8, 3136, 1024], P('section', 'dev')
- input_grad: bfloat16 [8, 50176, 256], P('section', 'dev')
- grad_expand: float32 [8, 256, 1024], P('section')
- grad_reduce: float32 [8, 1024, 256], P('section')
The draws below stay inside these ranges and needn't reach their ends.
All inputs are finite; a program needn't handle non-finite values.
Results may differ from the reference program's by a relative error of at most 0.02.
Values may be sent and summed in bfloat16 or wider, within the bound.
A program may use at most 128 MiB of HBM per device.

```python
import math
import jax
import jax.numpy as jnp
from jax import lax

CE = 256
FE = 1024
CL = 1024
FL = 4096
SECTIONS = 8
HID_DEV = 128
E_ROWS = 50176
L_ROWS = 3136
N_DEV = 32


def scaled_rows(key, leading):
    keys = jax.random.split(key, 4)
    shape = (leading, L_ROWS, CL)
    base = jnp.clip(jax.random.normal(keys[0], shape, jnp.float32), -4.0, 4.0)
    weight = 0.5
    rise = 6.0
    trend = jnp.exp(math.log(rise) * jnp.arange(L_ROWS, dtype=jnp.float32) / L_ROWS).reshape(1, L_ROWS, 1)
    row_factor = jnp.exp(jax.random.uniform(keys[1], (leading, L_ROWS, 1), jnp.float32, 0.0, math.log(2.0)))
    column_factor = jnp.exp(jax.random.uniform(keys[2], (leading, 1, CL), jnp.float32, 0.0, math.log(10.0)))
    offset = jnp.clip(jax.random.normal(keys[3], (leading, 1, CL), jnp.float32), -2.0, 2.0) * weight
    return 0.005 * (base * row_factor + offset) * trend * column_factor


def draw_late_sent(key, part):
    return scaled_rows(jax.random.fold_in(key, 101), SECTIONS).astype(jnp.bfloat16)


def draw_entry_rows(key, part):
    return scaled_rows(jax.random.fold_in(key, 202), 1)[0].astype(jnp.bfloat16)


def block_scale(own_key, shape, shards, smallest, top_value):
    loudness = 1.0
    for position, parts in shards:
        steps = jax.random.uniform(jax.random.fold_in(jax.random.fold_in(own_key, 6), position), (parts,), jnp.float32, smallest / len(shards), top_value / len(shards))
        loudness = loudness * jnp.repeat(jnp.exp(steps), shape[position] // parts).reshape((-1,) + (1,) * (len(shape) - 1 - position))
    return loudness


def scatter_about(own_key, extent, deviation, reach, cuts=(), held_as=jnp.bfloat16):
    values = jax.random.normal(own_key, extent, jnp.float32) * deviation
    if len(cuts) > 0:
        values = block_scale(own_key, extent, cuts, -0.22, 0.18) * values
    return jnp.clip(values, min=-reach, max=reach).astype(held_as)


def setup_inputs(seed: int = 0) -> dict:
    key_of = jax.random.split(jax.random.key(seed), 14)
    return {
        "late_sent": draw_late_sent(jax.random.fold_in(key_of[13], 71), 0),
        "entry_rows": draw_entry_rows(jax.random.fold_in(key_of[13], 71), 0),
        "gain_first": jnp.clip(1.0 + 0.18 * jax.random.normal(key_of[2], (SECTIONS, CL), jnp.float32), 0.1, 1.9),
        "shift_first": scatter_about(key_of[3], (SECTIONS, CL), 0.5, 3.0, ((0, 8),), jnp.float32),
        "expand_late": scatter_about(key_of[4], (SECTIONS, CL, FL), CL ** -0.5, 0.1875, ((0, 8), (2, 32))),
        "gain_inner": jnp.clip(1.0 + 0.18 * jax.random.normal(key_of[5], (SECTIONS, FL), jnp.float32), 0.1, 1.9),
        "shift_inner": scatter_about(key_of[6], (SECTIONS, FL), 0.5, 3.0, ((0, 8), (1, 32)), jnp.float32),
        "reduce_late": scatter_about(key_of[7], (SECTIONS, FL, CL), FL ** -0.5, 0.09375, ((0, 8), (1, 32))),
        "early_saved": scatter_about(key_of[8], (SECTIONS, E_ROWS, CE), 1.0, 6.0, ((0, 8), (1, 32))),
        "upstream_grad": scatter_about(key_of[9], (SECTIONS, E_ROWS, CE), 1.0, 6.0, ((0, 8), (1, 32))),
        "exit_grad": scatter_about(key_of[10], (E_ROWS, CE), 1.0, 6.0, ((0, 32),)),
        "expand_early": scatter_about(key_of[11], (SECTIONS, CE, FE), CE ** -0.5, 0.375, ((0, 8),)),
        "reduce_early": scatter_about(key_of[12], (SECTIONS, FE, CE), FE ** -0.5, 0.1875, ((0, 8),)),
    }


epsilon = 1e-05

def affine(sums, squares, count, gain, shift):
    average = sums / count
    second = squares / count
    spread = gain * lax.rsqrt(second - average * average + epsilon)
    return (spread, shift - average * spread)

def silu_slope(values):
    sigma = jax.nn.sigmoid(values)
    return sigma * (1.0 + values * (1.0 - sigma))

def late_block(inputs, gain_first, shift_first, expand, gain_inner, shift_inner, reduce_weight):
    count = inputs.shape[0]
    values = inputs.astype(jnp.float32)
    spread, offset = affine(lax.optimization_barrier(jnp.sum(values, axis=0)), lax.optimization_barrier(jnp.sum(values * values, axis=0)), count, gain_first, shift_first)
    first = jax.nn.silu(values * spread + offset).astype(jnp.bfloat16)
    inner = jnp.dot(first, expand, preferred_element_type=jnp.float32)
    spread_two, offset_two = affine(lax.optimization_barrier(jnp.sum(inner, axis=0)), lax.optimization_barrier(jnp.sum(inner * inner, axis=0)), count, gain_inner, shift_inner)
    hidden = jax.nn.silu(inner * spread_two + offset_two).astype(jnp.bfloat16)

    def add_group(total, group):
        start = (group * HID_DEV).astype(jnp.int32)
        term = jnp.dot(lax.dynamic_slice_in_dim(hidden, start, HID_DEV, 1), lax.dynamic_slice_in_dim(reduce_weight, start, HID_DEV, 0), preferred_element_type=jnp.float32)
        rounded = lax.optimization_barrier(term.astype(jnp.bfloat16))
        return (total + rounded.astype(jnp.float32), None)
    total, unused = lax.scan(add_group, jnp.zeros((count, CL), jnp.float32), jnp.arange(N_DEV, dtype=jnp.int32))
    return (values + total).astype(jnp.bfloat16)

def early_block(saved, grad, expand, reduce_weight):
    pre = jnp.dot(saved, expand, preferred_element_type=jnp.float32)
    hidden = jax.nn.silu(pre).astype(jnp.bfloat16)
    back = lax.dot_general(grad, reduce_weight, (((1,), (1,)), ((), ())), preferred_element_type=jnp.float32)
    slope = (back * silu_slope(pre)).astype(jnp.bfloat16)
    result = grad.astype(jnp.float32) + lax.dot_general(slope, expand, (((1,), (1,)), ((), ())), preferred_element_type=jnp.float32)
    grad_expand = lax.dot_general(saved, slope, (((0,), (0,)), ((), ())), preferred_element_type=jnp.float32)
    grad_reduce = lax.dot_general(hidden, grad, (((0,), (0,)), ((), ())), preferred_element_type=jnp.float32)
    return (result.astype(jnp.bfloat16), grad_expand, grad_reduce)

def reference(late_sent, entry_rows, gain_first, shift_first, expand_late, gain_inner, shift_inner, reduce_late, early_saved, upstream_grad, exit_grad, expand_early, reduce_early):
    late_in = jnp.concatenate([entry_rows[None], late_sent[:-1]], axis=0)
    grad_in = jnp.concatenate([upstream_grad[1:], exit_grad[None]], axis=0)
    late_out = lax.map(lambda items: late_block(*items), (late_in, gain_first, shift_first, expand_late, gain_inner, shift_inner, reduce_late))
    input_grad, grad_expand, grad_reduce = lax.map(lambda items: early_block(*items), (early_saved, grad_in, expand_early, reduce_early))
    factor = 1.0 / math.sqrt(E_ROWS)
    return (late_out, input_grad, grad_expand * factor, grad_reduce * factor)
```

```python
import functools
import math

import jax
import jax.numpy as jnp
from jax import lax
from jax.experimental import pallas as pl
from jax.experimental.pallas import tpu as pltpu
from jax.sharding import Mesh
from jax.sharding import PartitionSpec as P

DEV = ("b", "z", "c")
MESH = pl.DeviceIdType.MESH
F32 = jnp.float32
BF16 = jnp.bfloat16
EPS = 1e-05
Q = 4
PIECES = 7
BLOCK = 256
N_SEMS = 320


def silu(v):
    return v * jax.nn.sigmoid(v)


def affine(sums, squares, count, gain, shift):
    average = sums / count
    second = squares / count
    spread = gain * lax.rsqrt(second - average * average + EPS)
    return spread, shift - average * spread


def kernel(
    sizes,
    late_ref,
    entry_ref,
    gain_first_ref,
    shift_first_ref,
    expand_late_ref,
    gain_inner_ref,
    shift_inner_ref,
    reduce_late_ref,
    saved_ref,
    up_ref,
    exit_ref,
    expand_early_ref,
    reduce_early_ref,
    late_out_ref,
    input_grad_ref,
    grads_ref,
    S,
    ZST,
    ZT,
    FST,
    GS,
    G,
    F,
    W1,
    W2,
    GI,
    SI,
    IST,
    INN,
    PT,
    SC,
    SA,
    RC,
    RA,
    LO,
    SV,
    GR,
    WE1,
    WE2,
    ACT,
    DS,
    OG,
    ACC,
    SD,
    RD,
    SX,
    RX,
    TF,
    SZ,
    RZ,
    FIN,
    sems,
):
    NS, NZ = sizes
    H = NZ // 2
    rows, CL = S.shape
    CQ = CL // Q
    HID = expand_late_ref.shape[1]
    e_rows, CE = SV.shape
    FE = WE1.shape[1]
    PR = e_rows // PIECES
    ZR = CE // 2 // NZ
    late_count = rows * NZ * 4

    s = lax.axis_index("section")
    b = lax.axis_index("b")
    z = lax.axis_index("z")
    c = lax.axis_index("c")
    ahead = lax.rem(s + 1, NS)
    behind = lax.rem(s + NS - 1, NS)
    other_b = 1 - b
    other_c = 1 - c

    def zat(d):
        return lax.rem(z + d + NZ, NZ)

    def group(k):
        where = {}
        if k & 2:
            where["b"] = other_b
        if k & 1:
            where["c"] = other_c
        return where

    used = [0]
    sent = []

    def new_sem():
        used[0] += 1
        return sems.at[used[0] - 1]

    def remote(src, dst, to, pair=None):
        pair = pair or (new_sem(), new_sem())
        return pltpu.make_async_remote_copy(
            src_ref=src, dst_ref=dst, send_sem=pair[0], recv_sem=pair[1], device_id=to, device_id_type=MESH
        )

    def send(src, dst, to):
        copy = remote(src, dst, to)
        copy.start()
        sent.append(copy)
        return copy

    def send_either(condition, one, two, dst, to):
        pair = (new_sem(), new_sem())
        first, second = remote(one, dst, to, pair), remote(two, dst, to, pair)

        @pl.when(condition)
        def _():
            first.start()

        @pl.when(jnp.logical_not(condition))
        def _():
            second.start()

        sent.append(first)
        return first

    def load(src, dst):
        copy = pltpu.make_async_copy(src, dst, new_sem())
        copy.start()
        return copy

    def cols(q):
        return slice(q * CQ, (q + 1) * CQ)

    barrier = pltpu.get_barrier_semaphore()
    greeted = [{"z": zat(d)} for d in range(1, NZ)] + [group(k) for k in (1, 2, 3)]
    greeted += [{"section": ahead, **group(k)} for k in range(4)]
    greeted += [{"section": behind, **group(k)} for k in range(4)]
    for to in greeted:
        pl.semaphore_signal(barrier, inc=1, device_id=to, device_id_type=MESH)

    last = s == NS - 1
    sem_s = new_sem()
    take_late = pltpu.make_async_copy(late_ref, S, sem_s)
    take_entry = pltpu.make_async_copy(entry_ref, S, sem_s)

    @pl.when(last)
    def _():
        take_entry.start()

    @pl.when(jnp.logical_not(last))
    def _():
        take_late.start()

    load_saved = load(saved_ref, SV)
    load_we1 = load(expand_early_ref, WE1)
    load_we2 = load(reduce_early_ref, WE2)
    load_gf = load(gain_first_ref, GS.at[0])
    load_sf = load(shift_first_ref, GS.at[1])
    load_w1 = load(expand_late_ref, W1.at[:, 0:HID])
    load_w2 = load(reduce_late_ref, W2.at[0:HID, :])
    load_gi = load(gain_inner_ref, GI.at[0])
    load_si = load(shift_inner_ref, SI.at[0])

    take_late.wait()
    for q in range(Q):
        values = S[:, cols(q)].astype(F32)
        ZST[0, 0:1, cols(q)] = jnp.sum(values, axis=0, keepdims=True)
        ZST[0, 1:2, cols(q)] = jnp.sum(values * values, axis=0, keepdims=True)

    pl.semaphore_wait(barrier, len(greeted))

    shift_late = [
        send_either(last, entry_ref.at[:, cols(q)], late_ref.at[:, cols(q)], G.at[0, :, cols(q)], {"section": ahead})
        for q in range(Q)
    ]
    z_stats = [send(ZST.at[0], ZST.at[d], {"z": zat(d)}) for d in range(1, NZ)]

    w1_near = send(expand_late_ref, W1.at[:, HID : 2 * HID], group(1))
    w1_far = send(expand_late_ref, W1.at[:, 2 * HID : 3 * HID], group(2))
    gains = []
    for k in (1, 2, 3):
        gains.append(send(gain_inner_ref, GI.at[k], group(k)))
        gains.append(send(shift_inner_ref, SI.at[k], group(k)))

    grad_pairs = [(new_sem(), new_sem()) for _ in range(PIECES)]
    first_grad = s == 0
    for p in range(PIECES):
        piece = slice(p * PR, (p + 1) * PR)
        one = remote(exit_ref.at[piece], GR.at[piece], {"section": behind}, grad_pairs[p])
        two = remote(up_ref.at[piece], GR.at[piece], {"section": behind}, grad_pairs[p])
        pl.when(first_grad)(one.start)
        pl.when(jnp.logical_not(first_grad))(two.start)
        sent.append(two)
    shift_grad = sent[-PIECES:]

    w2_near = send(reduce_late_ref, W2.at[HID : 2 * HID, :], group(1))
    w2_far = send(reduce_late_ref, W2.at[2 * HID : 3 * HID, :], group(2))

    load_saved.wait()
    load_we1.wait()
    load_we2.wait()

    def early_rows(p):
        return pl.ds(pl.multiple_of(p * PR, PR), PR)

    def early_one(p, carry):
        at = early_rows(p)
        saved = SV[at, :]
        for f in range(0, FE, BLOCK):
            pre = jnp.dot(saved, WE1[:, f : f + BLOCK], preferred_element_type=F32)
            sigma = jax.nn.sigmoid(pre)
            ACT[at, f : f + BLOCK] = (pre * sigma).astype(BF16)
            DS[at, f : f + BLOCK] = sigma * (1.0 + pre * (1.0 - sigma))
        return carry

    lax.fori_loop(0, PIECES, early_one, 0)

    ACC[...] = jnp.zeros(ACC.shape, F32)

    def early_two(p):
        at = slice(p * PR, (p + 1) * PR)
        shift_grad[p].wait_recv()
        grad = GR[at, :]
        saved = SV[at, :]
        result = grad.astype(F32)
        for f in range(0, FE, BLOCK):
            block = slice(f, f + BLOCK)
            back = lax.dot_general(grad, WE2[block, :], (((1,), (1,)), ((), ())), preferred_element_type=F32)
            slope = (back * DS[at, block]).astype(BF16)
            ACC[0, :, block] += lax.dot_general(saved, slope, (((0,), (0,)), ((), ())), preferred_element_type=F32)
            ACC[1, :, block] += lax.dot_general(
                grad, ACT[at, block], (((0,), (0,)), ((), ())), preferred_element_type=F32
            )
            result += lax.dot_general(slope, WE1[:, block], (((1,), (1,)), ((), ())), preferred_element_type=F32)
        OG[at, :] = result.astype(BF16)
        return load(OG.at[at], input_grad_ref.at[at])

    hops_c, hops_a = [], []

    def forward(t, q):
        if t < H or q < Q // 2:
            hops_c.append((t, q, send(G.at[t - 1, :, cols(q)], G.at[t, :, cols(q)], {"z": zat(1)})))
        if t < H or q >= Q // 2:
            src, dst = (NZ - t + 1) % NZ, NZ - t
            hops_a.append((t, q, send(G.at[src, :, cols(q)], G.at[dst, :, cols(q)], {"z": zat(-1)})))

    def arrived(t, q):
        for hops in (hops_c, hops_a):
            for u, r, copy in hops:
                if (u, r) == (t, q):
                    copy.wait_recv()

    for q in range(Q):
        shift_late[q].wait_recv()
        forward(1, q)

    for copy in z_stats:
        copy.wait_recv()
    total = ZST[0]
    for d in range(1, NZ):
        total = total + ZST[d]
    ZT[...] = total
    first_stats = [send(ZT, FST.at[k], {"section": ahead, **group(k)}) for k in range(4)]

    if H > 1:
        for q in range(Q):
            arrived(1, q)
            forward(2, q)

    for copy in first_stats:
        copy.wait_recv()
    load_gf.wait()
    load_sf.wait()
    sums = FST[0] + FST[1] + FST[2] + FST[3]
    spread, offset = affine(sums[0:1], sums[1:2], late_count, GS[0], GS[1])

    def first_of(slot):
        for q in range(Q):
            at = cols(q)
            values = G[slot, :, at].astype(F32) * spread[:, at] + offset[:, at]
            F[slot, :, at] = silu(values).astype(BF16)

    stats = [0.0, 0.0]

    def inner_of(slot):
        inner = jnp.dot(F[slot], W1[...], preferred_element_type=F32)
        INN[slot] = inner
        stats[0] += jnp.sum(inner, axis=0, keepdims=True)
        stats[1] += jnp.sum(inner * inner, axis=0, keepdims=True)

    first_of(0)
    done = []
    for t in range(2, H):
        for q in range(Q):
            arrived(t, q)
            forward(t + 1, q)
        for slot in (t - 1, NZ - t + 1):
            first_of(slot)
            done.append(slot)

    w1_far.wait_recv()
    w1_fwd = send(W1.at[:, 2 * HID : 3 * HID], W1.at[:, 3 * HID :], group(1))
    load_w1.wait()
    w1_near.wait_recv()
    w1_fwd.wait_recv()
    for slot in [0] + done:
        inner_of(slot)
    for slot in (H - 1, H + 1):
        if slot not in done and slot != 0 and H > 1:
            first_of(slot)
            inner_of(slot)
    for q in range(Q):
        arrived(H, q)
    first_of(H)
    inner_of(H)

    IST[0, 0:1] = stats[0]
    IST[0, 1:2] = stats[1]
    inner_stats = [send(IST.at[0], IST.at[k], group(k)) for k in (1, 2, 3)]

    out_grads = []
    for p in range(PIECES // 2):
        out_grads.append(early_two(p))

    w2_far.wait_recv()
    w2_fwd = send(W2.at[2 * HID : 3 * HID, :], W2.at[3 * HID :, :], group(1))
    load_w2.wait()
    load_gi.wait()
    load_si.wait()
    w2_near.wait_recv()
    for copy in gains:
        copy.wait_recv()
    for copy in inner_stats:
        copy.wait_recv()
    spreads, offsets = [], []
    for k in range(4):
        piece = IST[0, :, k * HID : (k + 1) * HID]
        for d in (1, 2, 3):
            j = k ^ d
            piece = piece + IST[d, :, j * HID : (j + 1) * HID]
        one, two = affine(piece[0:1], piece[1:2], late_count, GI[k], SI[k])
        spreads.append(one)
        offsets.append(two)
    spread_two = jnp.concatenate(spreads, axis=1)
    offset_two = jnp.concatenate(offsets, axis=1)
    w2_fwd.wait_recv()

    def partial_of(slot):
        hidden = silu(INN[slot] * spread_two + offset_two).astype(BF16)
        PT[slot] = jnp.dot(hidden, W2[...], preferred_element_type=F32)

    sums_c, sums_a = {}, {}

    def sum_hop(t):
        for q in range(Q):
            at = cols(q)
            for slot, sums_d, S_, R_, step, half in (
                (NZ - (H - t), sums_c, SC, RC, 1, q < Q // 2),
                (H - t, sums_a, SA, RA, -1, q >= Q // 2),
            ):
                if t == 0 and not half:
                    continue
                value = PT[slot, :, at]
                if t > 1 or (t == 1 and half):
                    sums_d[t - 1, q].wait_recv()
                    value = value + R_[t - 1, :, at].astype(F32)
                S_[t, :, at] = value.astype(BF16)
                sums_d[t, q] = send(S_.at[t, :, at], R_.at[t, :, at], {"z": zat(step)})

    partial_of(H)
    sum_hop(0)
    for t in range(1, H):
        partial_of(NZ - (H - t))
        partial_of(H - t)
        sum_hop(t)
        if t == 1:
            for p in range(PIECES // 2, PIECES):
                out_grads.append(early_two(p))
            for half in (0, 1):
                h = other_b if half == 0 else b
                at = pl.ds(pl.multiple_of(h * (CE // 2), CE // 2), CE // 2)
                SD[h] = ACC[other_c, at, :].astype(BF16)
            pair_sums = [send(SD.at[h], RD.at[h], group(1)) for h in (other_b, b)]
    partial_of(0)

    half_other = pl.ds(pl.multiple_of(other_b * (CE // 2), CE // 2), CE // 2)
    half_own = pl.ds(pl.multiple_of(b * (CE // 2), CE // 2), CE // 2)
    pair_sums[0].wait_recv()
    pair_sums[1].wait_recv()
    SX[...] = (ACC[c, half_other, :] + RD[other_b].astype(F32)).astype(BF16)
    x_sum = send(SX, RX, group(2))

    for q in range(Q):
        at = cols(q)
        if H > 1 or q < Q // 2:
            sums_c[H - 1, q].wait_recv()
        if H > 1 or q >= Q // 2:
            sums_a[H - 1, q].wait_recv()
        value = PT[0, :, at]
        if H > 1 or q < Q // 2:
            value = value + RC[H - 1, :, at].astype(F32)
        if H > 1 or q >= Q // 2:
            value = value + RA[H - 1, :, at].astype(F32)
        LO[:, at] = (G[0, :, at].astype(F32) + value).astype(BF16)
    out_late = load(LO, late_out_ref)

    x_sum.wait_recv()
    TF[...] = ACC[c, half_own, :] + RD[b].astype(F32) + RX[...].astype(F32)
    SZ[...] = TF[...].astype(BF16)

    def zrows(i):
        return pl.ds(pl.multiple_of(i * ZR, ZR), ZR)

    z_sums = [send(SZ.at[zrows(zat(d))], RZ.at[d], {"z": zat(d)}) for d in range(1, NZ)]
    value = TF[zrows(z), :]
    for d, copy in enumerate(z_sums, 1):
        copy.wait_recv()
        value = value + RZ[d].astype(F32)
    factor = 1.0 / math.sqrt(e_rows * NZ * 4)
    FIN[c, b, zrows(z), :] = (value * factor).astype(BF16)
    own = FIN.at[c, b, zrows(z)]
    z_back = [send(own, own, {"z": zat(d)}) for d in range(1, NZ)]
    for copy in z_back:
        copy.wait_recv()
    x_back = send(FIN.at[c, b], FIN.at[c, b], group(2))
    c_back = send(FIN.at[c, b], FIN.at[c, b], group(1))
    x_back.wait_recv()
    c_back_two = send(FIN.at[c, other_b], FIN.at[c, other_b], group(1))
    c_back.wait_recv()
    c_back_two.wait_recv()
    out_fin = load(FIN, grads_ref)

    for copy in sent:
        copy.wait_send()
    for copy in out_grads:
        copy.wait()
    out_late.wait()
    out_fin.wait()


def shards(
    late_sent,
    entry_rows,
    gain_first,
    shift_first,
    expand_late,
    gain_inner,
    shift_inner,
    reduce_late,
    early_saved,
    upstream_grad,
    exit_grad,
    expand_early,
    reduce_early,
):
    rows, CL = entry_rows.shape
    e_rows, CE = exit_grad.shape
    FE = expand_early.shape[2]
    HID = expand_late.shape[2]
    NS, NZ = lax.axis_size("section"), lax.axis_size("z")
    H = NZ // 2
    VM = pltpu.VMEM
    scratch = [
        VM((rows, CL), BF16),
        VM((NZ, 2, CL), F32),
        VM((2, CL), F32),
        VM((4, 2, CL), F32),
        VM((2, 1, CL), F32),
        VM((NZ, rows, CL), BF16),
        VM((NZ, rows, CL), BF16),
        VM((CL, 4 * HID), BF16),
        VM((4 * HID, CL), BF16),
        VM((4, 1, HID), F32),
        VM((4, 1, HID), F32),
        VM((4, 2, 4 * HID), F32),
        VM((NZ, rows, 4 * HID), F32),
        VM((NZ, rows, CL), F32),
        VM((H, rows, CL), BF16),
        VM((H, rows, CL), BF16),
        VM((H, rows, CL), BF16),
        VM((H, rows, CL), BF16),
        VM((rows, CL), BF16),
        VM((e_rows, CE), BF16),
        VM((e_rows, CE), BF16),
        VM((CE, FE), BF16),
        VM((FE, CE), BF16),
        VM((e_rows, FE), BF16),
        VM((e_rows, FE), F32),
        VM((e_rows, CE), BF16),
        VM((2, CE, FE), F32),
        VM((2, CE // 2, FE), BF16),
        VM((2, CE // 2, FE), BF16),
        VM((CE // 2, FE), BF16),
        VM((CE // 2, FE), BF16),
        VM((CE // 2, FE), F32),
        VM((CE // 2, FE), BF16),
        VM((NZ, CE // 2 // NZ, FE), BF16),
        VM((2, 2, CE // 2, FE), BF16),
        pltpu.SemaphoreType.DMA((N_SEMS,)),
    ]
    anywhere = pl.BlockSpec(memory_space=pl.ANY)
    late_out, input_grad, grads = pl.pallas_call(
        functools.partial(kernel, (NS, NZ)),
        out_shape=(
            jax.ShapeDtypeStruct((rows, CL), BF16),
            jax.ShapeDtypeStruct((e_rows, CE), BF16),
            jax.ShapeDtypeStruct((2, 2, CE // 2, FE), BF16),
        ),
        in_specs=[anywhere] * 13,
        out_specs=(anywhere,) * 3,
        scratch_shapes=scratch,
        compiler_params=pltpu.CompilerParams(
            collective_id=0, has_side_effects=True, vmem_limit_bytes=60 * 1024 * 1024
        ),
        name="relay_step",
    )(
        late_sent[0],
        entry_rows,
        gain_first,
        shift_first,
        expand_late[0],
        gain_inner,
        shift_inner,
        reduce_late[0],
        early_saved[0],
        upstream_grad[0],
        exit_grad,
        expand_early[0],
        reduce_early[0],
    )
    grads = grads.reshape(2, CE, FE)
    return (
        late_out[None],
        input_grad[None],
        grads[0].astype(F32)[None],
        grads[1].T.astype(F32)[None],
    )


def solution(mesh):
    sections, devices = mesh.devices.shape
    split = Mesh(mesh.devices.reshape(sections, 2, devices // 4, 2), ("section", *DEV))
    return jax.shard_map(
        shards,
        mesh=split,
        in_specs=(
            P("section", DEV, None),
            P(DEV, None),
            P("section", None),
            P("section", None),
            P("section", None, DEV),
            P("section", DEV),
            P("section", DEV),
            P("section", DEV, None),
            P("section", DEV, None),
            P("section", DEV, None),
            P(DEV, None),
            P("section", None, None),
            P("section", None, None),
        ),
        out_specs=(
            P("section", DEV, None),
            P("section", DEV, None),
            P("section", None, None),
            P("section", None, None),
        ),
        check_vma=False,
    )
```

```python
import functools
import math

import jax
import jax.numpy as jnp
from jax import lax
from jax.experimental import pallas as pl
from jax.experimental.pallas import tpu as pltpu
from jax.sharding import Mesh
from jax.sharding import PartitionSpec as P

DEV = ("b", "z", "c")
MESH = pl.DeviceIdType.MESH
F32 = jnp.float32
BF16 = jnp.bfloat16
EPS = 1e-05
Q = 4
PIECES = 7
BLOCK = 256
N_SEMS = 400
W2_AT = 2
EARLY_FIRST = 3
HELD = 4
PLAN = "mmmmmmmmm" + "msmmsms" + "msmssssmssm" + "mmmsm" + "msmmm"
FAR_FIRST = (4, 3, 5, 2, 6, 1, 7, 0)


def silu(v):
    return v * jax.nn.sigmoid(v)


def affine(sums, squares, count, gain, shift):
    average = sums / count
    second = squares / count
    spread = gain * lax.rsqrt(second - average * average + EPS)
    return spread, shift - average * spread


def kernel(
    sizes,
    late_ref,
    entry_ref,
    gain_first_ref,
    shift_first_ref,
    expand_late_ref,
    gain_inner_ref,
    shift_inner_ref,
    reduce_late_ref,
    saved_ref,
    up_ref,
    exit_ref,
    expand_early_ref,
    reduce_early_ref,
    LO,
    OG,
    GE,
    OR,
    S,
    ZST,
    ZT,
    FST,
    GS,
    G,
    F,
    W1,
    W2,
    GI,
    SI,
    IST,
    INN,
    PT,
    SC,
    SA,
    RC,
    RA,
    SV,
    GR,
    WE1,
    WE2,
    ACT,
    DS,
    ACC,
    SD,
    RD,
    SX,
    RX,
    TF,
    SZ,
    RZ,
    FIN,
    sems,
):
    NS, NZ = sizes
    H = NZ // 2
    rows, CL = S.shape
    CQ = CL // Q
    HID = expand_late_ref.shape[1]
    e_rows, CE = SV.shape
    FE = WE1.shape[1]
    PR = e_rows // PIECES
    ZR = CE // 2 // NZ
    late_count = rows * NZ * 4

    s = lax.axis_index("section")
    b = lax.axis_index("b")
    z = lax.axis_index("z")
    c = lax.axis_index("c")
    ahead = lax.rem(s + 1, NS)
    behind = lax.rem(s + NS - 1, NS)
    other_b = 1 - b
    other_c = 1 - c

    def zat(d):
        return lax.rem(z + d + NZ, NZ)

    def group(k):
        where = {}
        if k & 2:
            where["b"] = other_b
        if k & 1:
            where["c"] = other_c
        return where

    used = [0]
    sent = []

    def new_sem():
        used[0] += 1
        return sems.at[used[0] - 1]

    def remote(src, dst, to, pair=None):
        pair = pair or (new_sem(), new_sem())
        return pltpu.make_async_remote_copy(
            src_ref=src, dst_ref=dst, send_sem=pair[0], recv_sem=pair[1], device_id=to, device_id_type=MESH
        )

    def send(src, dst, to):
        copy = remote(src, dst, to)
        copy.start()
        sent.append(copy)
        return copy

    def load(src, dst):
        copy = pltpu.make_async_copy(src, dst, new_sem())
        copy.start()
        return copy

    def cols(q):
        return slice(q * CQ, (q + 1) * CQ)

    barrier = pltpu.get_barrier_semaphore()
    greeted = [{"z": zat(d)} for d in range(1, NZ)] + [group(k) for k in (1, 2, 3)]
    greeted += [{"section": ahead, **group(k)} for k in range(4)]
    greeted += [{"section": behind, **group(k)} for k in range(4)]
    with jax.named_scope("greet"):
        for to in greeted:
            pl.semaphore_signal(barrier, inc=1, device_id=to, device_id_type=MESH)

    last = s == NS - 1
    sem_s = new_sem()
    take_late = pltpu.make_async_copy(late_ref, S, sem_s)
    take_entry = pltpu.make_async_copy(entry_ref, S, sem_s)

    @pl.when(last)
    def _():
        take_entry.start()

    @pl.when(jnp.logical_not(last))
    def _():
        take_late.start()

    load_saved = load(saved_ref, SV)
    load_we1 = load(expand_early_ref, WE1)
    load_we2 = load(reduce_early_ref, WE2)
    load_gf = load(gain_first_ref, GS.at[0])
    load_sf = load(shift_first_ref, GS.at[1])
    load_w1 = load(expand_late_ref, W1.at[:, 0:HID])
    load_w2 = load(reduce_late_ref, W2.at[0:HID, :])
    load_gi = load(gain_inner_ref, GI.at[0])
    load_si = load(shift_inner_ref, SI.at[0])

    with jax.named_scope("own_stats"):
        take_late.wait()
        for q in range(Q):
            values = S[:, cols(q)].astype(F32)
            ZST[0, 0:1, cols(q)] = jnp.sum(values, axis=0, keepdims=True)
            ZST[0, 1:2, cols(q)] = jnp.sum(values * values, axis=0, keepdims=True)

    with jax.named_scope("barrier"):
        pl.semaphore_wait(barrier, len(greeted))

    with jax.named_scope("sends"):
        shift_late = [send(S.at[:, cols(q)], G.at[0, :, cols(q)], {"section": ahead}) for q in range(Q)]
        z_stats = [send(ZST.at[0], ZST.at[d], {"z": zat(d)}) for d in range(1, NZ)]

        w1_near = send(expand_late_ref, W1.at[:, HID : 2 * HID], group(1))
        w2_near = send(reduce_late_ref, W2.at[HID : 2 * HID, :], group(1))
        gains = []
        for k in (1, 2, 3):
            gains.append(send(gain_inner_ref, GI.at[k], group(k)))
            gains.append(send(shift_inner_ref, SI.at[k], group(k)))

    first_grad = s == 0
    shift_grad = []
    for p in range(PIECES):
        piece = slice(p * PR, (p + 1) * PR)
        pair = (new_sem(), new_sem())
        one = remote(exit_ref.at[piece], GR.at[piece], {"section": behind}, pair)
        two = remote(up_ref.at[piece], GR.at[piece], {"section": behind}, pair)
        shift_grad.append((one, two))

    def start_grad(p):
        one, two = shift_grad[p]
        pl.when(first_grad)(one.start)
        pl.when(jnp.logical_not(first_grad))(two.start)
        sent.append(two)

    w1_far = remote(expand_late_ref, W1.at[:, 2 * HID : 3 * HID], group(2))
    w2_far = remote(reduce_late_ref, W2.at[2 * HID : 3 * HID, :], group(2))

    def start_far(copy):
        copy.start()
        sent.append(copy)

    bulk = [functools.partial(start_grad, p) for p in range(PIECES)]
    bulk.insert(W2_AT, functools.partial(start_far, w2_far))

    def tick(n=1, keep=0):
        for _ in range(n):
            if len(bulk) > keep:
                bulk.pop(0)()

    with jax.named_scope("load_wait"):
        load_saved.wait()
        load_we1.wait()
        load_we2.wait()

    def early_rows(p):
        return pl.ds(pl.multiple_of(p * PR, PR), PR)

    def early_one(p, carry):
        at = early_rows(p)
        saved = SV[at, :]
        for f in range(0, FE, BLOCK):
            pre = jnp.dot(saved, WE1[:, f : f + BLOCK], preferred_element_type=F32)
            sigma = jax.nn.sigmoid(pre)
            ACT[at, f : f + BLOCK] = (pre * sigma).astype(BF16)
            DS[at, f : f + BLOCK] = sigma * (1.0 + pre * (1.0 - sigma))
        return carry

    with jax.named_scope("early_one"):
        lax.fori_loop(0, PIECES, early_one, 0)

        ACC[...] = jnp.zeros(ACC.shape, F32)

    def early_two(p):
        at = slice(p * PR, (p + 1) * PR)
        with jax.named_scope("grad_wait"):
            shift_grad[p][1].wait_recv()
        with jax.named_scope("early_two"):
            grad = GR[at, :]
            saved = SV[at, :]
            result = grad.astype(F32)
            for f in range(0, FE, BLOCK):
                block = slice(f, f + BLOCK)
                back = lax.dot_general(grad, WE2[block, :], (((1,), (1,)), ((), ())), preferred_element_type=F32)
                slope = (back * DS[at, block]).astype(BF16)
                ACC[0, :, block] += lax.dot_general(saved, slope, (((0,), (0,)), ((), ())), preferred_element_type=F32)
                ACC[1, :, block] += lax.dot_general(
                    ACT[at, block], grad, (((0,), (0,)), ((), ())), preferred_element_type=F32
                )
                result += lax.dot_general(slope, WE1[:, block], (((1,), (1,)), ((), ())), preferred_element_type=F32)
            OG[at, :] = result.astype(BF16)

    hops_c, hops_a = [], []

    def forward(t, q):
        if t < H or q < Q // 2:
            hops_c.append((t, q, send(G.at[t - 1, :, cols(q)], G.at[t, :, cols(q)], {"z": zat(1)})))
        if t < H or q >= Q // 2:
            src, dst = (NZ - t + 1) % NZ, NZ - t
            hops_a.append((t, q, send(G.at[src, :, cols(q)], G.at[dst, :, cols(q)], {"z": zat(-1)})))

    def arrived(t, q):
        for hops in (hops_c, hops_a):
            for u, r, copy in hops:
                if (u, r) == (t, q):
                    copy.wait_recv()

    with jax.named_scope("zstats_wait"):
        for copy in z_stats:
            copy.wait_recv()
    total = ZST[0]
    for d in range(1, NZ):
        total = total + ZST[d]
    ZT[...] = total
    first_stats = [send(ZT, FST.at[k], {"section": ahead, **group(k)}) for k in range(4)]
    start_far(w1_far)
    tick()
    for q in range(Q):
        with jax.named_scope("shift_wait"):
            shift_late[q].wait_recv()
        forward(1, q)

    if H > 1:
        with jax.named_scope("hop1"):
            for q in range(Q):
                arrived(1, q)
                forward(2, q)
                if q % 2:
                    tick(keep=HELD)

    with jax.named_scope("fstats_wait"):
        for copy in first_stats:
            copy.wait_recv()
    load_gf.wait()
    load_sf.wait()
    sums = FST[0] + FST[1] + FST[2] + FST[3]
    spread, offset = affine(sums[0:1], sums[1:2], late_count, GS[0], GS[1])

    def first_of(slot):
        for q in range(Q):
            at = cols(q)
            values = G[slot, :, at].astype(F32) * spread[:, at] + offset[:, at]
            F[slot, :, at] = silu(values).astype(BF16)

    stats = [0.0, 0.0]

    def inner_of(slot):
        inner = jnp.dot(F[slot], W1[...], preferred_element_type=F32)
        INN[slot] = inner
        stats[0] += jnp.sum(inner, axis=0, keepdims=True)
        stats[1] += jnp.sum(inner * inner, axis=0, keepdims=True)

    def forward_w1():
        with jax.named_scope("w1_wait"):
            w1_far.wait_recv()
        return send(W1.at[:, 2 * HID : 3 * HID], W1.at[:, 3 * HID :], group(1))

    with jax.named_scope("first0"):
        first_of(0)
    done = []
    for t in range(2, H):
        with jax.named_scope(f"hop{t}"):
            for q in range(Q):
                arrived(t, q)
                forward(t + 1, q)
                if q % 2:
                    tick(keep=HELD)
        if t == 2:
            w1_fwd = forward_w1()
        for slot in (t - 1, NZ - t + 1):
            with jax.named_scope("first"):
                first_of(slot)
            done.append(slot)

    if H <= 2:
        w1_fwd = forward_w1()
    with jax.named_scope("w1_fwd_wait"):
        load_w1.wait()
        w1_near.wait_recv()
        w1_fwd.wait_recv()
    with jax.named_scope("inner5"):
        for slot in [0] + done:
            inner_of(slot)
    for slot in (H - 1, H + 1):
        if slot not in done and slot != 0 and H > 1:
            with jax.named_scope("first_inner"):
                first_of(slot)
                inner_of(slot)
    with jax.named_scope("hopH"):
        for q in range(Q):
            arrived(H, q)
    with jax.named_scope("first_inner"):
        first_of(H)
        inner_of(H)

    order = [d for d in FAR_FIRST if d < NZ]
    cuts = [(0, NZ // 2), (NZ // 2, NZ)]
    factor = 1.0 / math.sqrt(e_rows * NZ * 4)

    def acc_rows(half, d):
        return pl.ds(pl.multiple_of(half * (CE // 2) + zat(d) * ZR, ZR), ZR)

    pair_sums, x_sums, z_sums, z_back, x_back, c_back, c_back_two = {}, {}, {}, {}, {}, {}, {}

    def pair_send(h, k):
        lo, hi = cuts[k]
        for i in range(lo, hi):
            SD[h, i] = ACC[other_c, acc_rows(other_b if h == 0 else b, order[i]), :].astype(BF16)
        pair_sums[h, k] = send(SD.at[h, lo:hi], RD.at[h, lo:hi], group(1))

    def x_send(k):
        lo, hi = cuts[k]
        pair_sums[0, k].wait_recv()
        for i in range(lo, hi):
            SX[i] = (ACC[c, acc_rows(other_b, order[i]), :] + RD[0, i].astype(F32)).astype(BF16)
        x_sums[k] = send(SX.at[lo:hi], RX.at[lo:hi], group(2))

    def z_send(k):
        lo, hi = cuts[k]
        pair_sums[1, k].wait_recv()
        x_sums[k].wait_recv()
        for i in range(lo, hi):
            d = order[i]
            value = ACC[c, acc_rows(b, d), :] + RD[1, i].astype(F32) + RX[i].astype(F32)
            if d == 0:
                TF[...] = value
            else:
                SZ[d] = value.astype(BF16)
                z_sums[d] = send(SZ.at[d], RZ.at[d], {"z": zat(d)})

    def fin(core, half, d):
        return FIN.at[core, half, pl.ds(pl.multiple_of(zat(d) * ZR, ZR), ZR)]

    def back_to_x_and_core(d):
        piece = fin(c, b, d)
        x_back[d] = send(piece, piece, group(2))
        c_back[d] = send(piece, piece, group(1))

    def back_across(d):
        x_back[d].wait_recv()
        piece = fin(c, other_b, d)
        c_back_two[d] = send(piece, piece, group(1))

    def z_finish():
        value = TF[...]
        for d in order[::-1]:
            if d:
                z_sums[d].wait_recv()
                value = value + RZ[d].astype(F32)
        FIN[c, b, pl.ds(pl.multiple_of(z * ZR, ZR), ZR), :] = (value * factor).astype(BF16)
        own = fin(c, b, 0)
        for d in order[::-1]:
            if d:
                z_back[d] = send(own, own, {"z": zat(d)})
        back_to_x_and_core(0)

    def z_forward(d):
        z_back[d].wait_recv()
        back_to_x_and_core(-d)

    IST[0, 0:1] = stats[0]
    IST[0, 1:2] = stats[1]
    inner_stats = [send(IST.at[0], IST.at[k], group(k)) for k in (1, 2, 3)]

    tick(len(bulk))
    for p in range(EARLY_FIRST):
        early_two(p)

    with jax.named_scope("w2_wait"):
        w2_far.wait_recv()
    w2_fwd = send(W2.at[2 * HID : 3 * HID, :], W2.at[3 * HID :, :], group(1))
    with jax.named_scope("istats_wait"):
        load_w2.wait()
        load_gi.wait()
        load_si.wait()
        w2_near.wait_recv()
        for copy in gains:
            copy.wait_recv()
        for copy in inner_stats:
            copy.wait_recv()
    spreads, offsets = [], []
    for k in range(4):
        piece = IST[0, :, k * HID : (k + 1) * HID]
        for d in (1, 2, 3):
            j = k ^ d
            piece = piece + IST[d, :, j * HID : (j + 1) * HID]
        one, two = affine(piece[0:1], piece[1:2], late_count, GI[k], SI[k])
        spreads.append(one)
        offsets.append(two)
    spread_two = jnp.concatenate(spreads, axis=1)
    offset_two = jnp.concatenate(offsets, axis=1)
    with jax.named_scope("w2_fwd_wait"):
        w2_fwd.wait_recv()

    def partial_of(slot):
        hidden = silu(INN[slot] * spread_two + offset_two).astype(BF16)
        PT[slot] = jnp.dot(hidden, W2[...], preferred_element_type=F32)

    sums_c, sums_a = {}, {}

    def sum_hop(t, q):
        at = cols(q)
        for slot, sums_d, S_, R_, step, half in (
            (NZ - (H - t), sums_c, SC, RC, 1, q < Q // 2),
            (H - t, sums_a, SA, RA, -1, q >= Q // 2),
        ):
            if t == 0 and not half:
                continue
            value = PT[slot, :, at]
            if t > 1 or (t == 1 and half):
                sums_d[t - 1, q].wait_recv()
                value = value + R_[t - 1, :, at].astype(F32)
            S_[t, :, at] = value.astype(BF16)
            sums_d[t, q] = send(S_.at[t, :, at], R_.at[t, :, at], {"z": zat(step)})

    def late_final(q):
        at = cols(q)
        value = PT[0, :, at]
        if H > 1 or q < Q // 2:
            sums_c[H - 1, q].wait_recv()
            value = value + RC[H - 1, :, at].astype(F32)
        if H > 1 or q >= Q // 2:
            sums_a[H - 1, q].wait_recv()
            value = value + RA[H - 1, :, at].astype(F32)
        LO[:, at] = (G[0, :, at].astype(F32) + value).astype(BF16)

    def partials(t):
        if t == 0:
            partial_of(H)
        elif t == H:
            partial_of(0)
        else:
            partial_of(NZ - (H - t))
            partial_of(H - t)

    near_first = [d for d in order[::-1] if d]
    side = [("early_two", functools.partial(early_two, p)) for p in range(EARLY_FIRST, PIECES)]
    side += [("pair_send", functools.partial(pair_send, h, k)) for h in (0, 1) for k in (0, 1)]
    side += [("x_send", functools.partial(x_send, k)) for k in (0, 1)]
    side += [("z_send", functools.partial(z_send, k)) for k in (0, 1)]
    side.append(("z_finish", z_finish))
    side += [("z_forward", functools.partial(z_forward, d)) for d in near_first[:2]]
    side.append(("across", functools.partial(back_across, 0)))
    for at, d in enumerate(near_first[2:]):
        side.append(("z_forward", functools.partial(z_forward, d)))
        if at:
            side.append(("across", functools.partial(back_across, -near_first[at - 1])))
    main = [("partials", functools.partial(partials, 0))]
    main += [("sum0", functools.partial(sum_hop, 0, q)) for q in range(Q)]
    main += [("partials", functools.partial(partials, t)) for t in range(1, H + 1)]
    main += [(f"sum{t}", functools.partial(sum_hop, t, q)) for t in range(1, H) for q in range(Q)]
    main += [("late_final", functools.partial(late_final, q)) for q in range(Q)]
    for step in PLAN:
        which = main if step == "m" else side
        if which:
            name, go = which.pop(0)
            with jax.named_scope(name):
                go()
    for name, go in main + side:
        with jax.named_scope(name):
            go()

    with jax.named_scope("across"):
        for d in near_first:
            if -d not in c_back_two:
                back_across(-d)
    with jax.named_scope("c_back"):
        for d in [0] + [-d for d in near_first]:
            c_back[d].wait_recv()
            c_back_two[d].wait_recv()
    with jax.named_scope("outputs"):
        for half in (0, 1):
            at = slice(half * (CE // 2), (half + 1) * (CE // 2))
            GE[at, :] = FIN[0, half].astype(F32)
            for f in range(0, FE, BLOCK):
                OR[f + half * (CE // 2) : f + (half + 1) * (CE // 2), :] = FIN[1, half, :, f : f + BLOCK].astype(F32)

    with jax.named_scope("drain"):
        for copy in sent:
            copy.wait_send()


def place(*refs):
    sems = refs[8]
    copies = [pltpu.make_async_copy(refs[i], refs[4 + i], sems.at[i]) for i in range(4)]
    for copy in copies:
        copy.start()
    for copy in copies:
        copy.wait()


def shards(
    late_sent,
    entry_rows,
    gain_first,
    shift_first,
    expand_late,
    gain_inner,
    shift_inner,
    reduce_late,
    early_saved,
    upstream_grad,
    exit_grad,
    expand_early,
    reduce_early,
):
    rows, CL = entry_rows.shape
    e_rows, CE = exit_grad.shape
    FE = expand_early.shape[2]
    HID = expand_late.shape[2]
    NS, NZ = lax.axis_size("section"), lax.axis_size("z")
    H = NZ // 2
    VM = pltpu.VMEM
    scratch = [
        VM((rows, CL), BF16),
        VM((NZ, 2, CL), F32),
        VM((2, CL), F32),
        VM((4, 2, CL), F32),
        VM((2, 1, CL), F32),
        VM((NZ, rows, CL), BF16),
        VM((NZ, rows, CL), BF16),
        VM((CL, 4 * HID), BF16),
        VM((4 * HID, CL), BF16),
        VM((4, 1, HID), F32),
        VM((4, 1, HID), F32),
        VM((4, 2, 4 * HID), F32),
        VM((NZ, rows, 4 * HID), F32),
        VM((NZ, rows, CL), F32),
        VM((H, rows, CL), BF16),
        VM((H, rows, CL), BF16),
        VM((H, rows, CL), BF16),
        VM((H, rows, CL), BF16),
        VM((e_rows, CE), BF16),
        VM((e_rows, CE), BF16),
        VM((CE, FE), BF16),
        VM((FE, CE), BF16),
        VM((e_rows, FE), BF16),
        VM((e_rows, FE), F32),
        VM((2, CE, FE), F32),
        VM((2, NZ, CE // 2 // NZ, FE), BF16),
        VM((2, NZ, CE // 2 // NZ, FE), BF16),
        VM((NZ, CE // 2 // NZ, FE), BF16),
        VM((NZ, CE // 2 // NZ, FE), BF16),
        VM((CE // 2 // NZ, FE), F32),
        VM((NZ, CE // 2 // NZ, FE), BF16),
        VM((NZ, CE // 2 // NZ, FE), BF16),
        VM((2, 2, CE // 2, FE), BF16),
        pltpu.SemaphoreType.DMA((N_SEMS,)),
    ]
    hbm = pl.BlockSpec(memory_space=pltpu.HBM)
    vmem = pl.BlockSpec(memory_space=pltpu.VMEM)
    late_out, input_grad, grad_expand, grad_reduce = pl.pallas_call(
        functools.partial(kernel, (NS, NZ)),
        out_shape=(
            VM((rows, CL), BF16),
            VM((e_rows, CE), BF16),
            VM((CE, FE), F32),
            VM((FE, CE), F32),
        ),
        in_specs=[hbm] * 13,
        out_specs=(vmem,) * 4,
        scratch_shapes=scratch,
        compiler_params=pltpu.CompilerParams(
            collective_id=0, has_side_effects=True, vmem_limit_bytes=44 * 1024 * 1024
        ),
        name="relay_step",
    )(
        *(
            pltpu.with_memory_space_constraint(x, pltpu.HBM)
            for x in (
                late_sent[0],
                entry_rows,
                gain_first,
                shift_first,
                expand_late[0],
                gain_inner,
                shift_inner,
                reduce_late[0],
                early_saved[0],
                upstream_grad[0],
                exit_grad,
                expand_early[0],
                reduce_early[0],
            )
        )
    )
    results = (late_out, input_grad, grad_expand, grad_reduce)
    results = pl.pallas_call(
        place,
        out_shape=tuple(jax.ShapeDtypeStruct(x.shape, x.dtype) for x in results),
        in_specs=[vmem] * 4,
        out_specs=(pl.BlockSpec(memory_space=pl.ANY),) * 4,
        scratch_shapes=[pltpu.SemaphoreType.DMA((4,))],
        compiler_params=pltpu.CompilerParams(vmem_limit_bytes=4 * 1024 * 1024),
        name="place",
    )(*results)
    return tuple(x[None] for x in results)


def solution(mesh):
    sections, devices = mesh.devices.shape
    split = Mesh(mesh.devices.reshape(sections, 2, devices // 4, 2), ("section", *DEV))
    return jax.shard_map(
        shards,
        mesh=split,
        in_specs=(
            P("section", DEV, None),
            P(DEV, None),
            P("section", None),
            P("section", None),
            P("section", None, DEV),
            P("section", DEV),
            P("section", DEV),
            P("section", DEV, None),
            P("section", DEV, None),
            P("section", DEV, None),
            P(DEV, None),
            P("section", None, None),
            P("section", None, None),
        ),
        out_specs=(
            P("section", DEV, None),
            P("section", DEV, None),
            P("section", None, None),
            P("section", None, None),
        ),
        check_vma=False,
    )
```

```python
import functools
import math

import jax
import jax.numpy as jnp
from jax import lax
from jax.experimental import pallas as pl
from jax.experimental.pallas import tpu as pltpu
from jax.sharding import Mesh
from jax.sharding import PartitionSpec as P

DEV = ("b", "z", "c")
MESH = pl.DeviceIdType.MESH
F32 = jnp.float32
BF16 = jnp.bfloat16
EPS = 1e-05
Q = 4
PIECES = 7
BLOCK = 256
N_SEMS = 400
PLAN = (
    "Z0 Z1 I W0",
    "B0 ZF W1 B1",
    "12 13 R1 A0",
    "20 21 22 R2",
    "A7 A1 23 30",
    "31 R3 A6 A2",
    "32 33 R4 A5",
    "A3 0f 1f 2f",
    "3f A4",
)
FAR_FIRST = (4, 3, 5, 2, 6, 1, 7, 0)


def silu(v):
    return v * jax.nn.sigmoid(v)


def affine(sums, squares, count, gain, shift):
    average = sums / count
    second = squares / count
    spread = gain * lax.rsqrt(second - average * average + EPS)
    return spread, shift - average * spread


def kernel(
    sizes,
    late_ref,
    entry_ref,
    gain_first_ref,
    shift_first_ref,
    expand_late_ref,
    gain_inner_ref,
    shift_inner_ref,
    reduce_late_ref,
    saved_ref,
    up_ref,
    exit_ref,
    expand_early_ref,
    reduce_early_ref,
    LO,
    OG,
    GE,
    OR,
    S,
    ZST,
    ZT,
    FST,
    GS,
    G,
    F,
    W1,
    W2,
    GI,
    SI,
    IST,
    INN,
    HB,
    PT,
    SC,
    SA,
    RC,
    RA,
    SV,
    GR,
    WE1,
    WE2,
    ACT,
    DS,
    ACC,
    SD,
    RD,
    SX,
    RX,
    TF,
    SZ,
    RZ,
    FIN,
    sems,
):
    NS, NZ = sizes
    H = NZ // 2
    rows, CL = S.shape
    CQ = CL // Q
    HID = expand_late_ref.shape[1]
    e_rows, CE = SV.shape
    FE = WE1.shape[1]
    PR = e_rows // PIECES
    ZR = CE // 2 // NZ
    late_count = rows * NZ * 4

    s = lax.axis_index("section")
    b = lax.axis_index("b")
    z = lax.axis_index("z")
    c = lax.axis_index("c")
    ahead = lax.rem(s + 1, NS)
    behind = lax.rem(s + NS - 1, NS)
    other_b = 1 - b
    other_c = 1 - c

    def zat(d):
        return lax.rem(z + d + NZ, NZ)

    def group(k):
        where = {}
        if k & 2:
            where["b"] = other_b
        if k & 1:
            where["c"] = other_c
        return where

    used = [0]
    sent = []

    def new_sem():
        used[0] += 1
        return sems.at[used[0] - 1]

    def remote(src, dst, to, pair=None):
        pair = pair or (new_sem(), new_sem())
        return pltpu.make_async_remote_copy(
            src_ref=src, dst_ref=dst, send_sem=pair[0], recv_sem=pair[1], device_id=to, device_id_type=MESH
        )

    def send(src, dst, to):
        copy = remote(src, dst, to)
        copy.start()
        sent.append(copy)
        return copy

    def load(src, dst):
        copy = pltpu.make_async_copy(src, dst, new_sem())
        copy.start()
        return copy

    def cols(q):
        return slice(q * CQ, (q + 1) * CQ)

    barrier = pltpu.get_barrier_semaphore()
    greeted = [{"z": zat(d)} for d in range(1, NZ)] + [group(k) for k in (1, 2, 3)]
    greeted += [{"section": ahead, **group(k)} for k in range(4)]
    greeted += [{"section": behind, **group(k)} for k in range(4)]
    with jax.named_scope("greet"):
        for to in greeted:
            pl.semaphore_signal(barrier, inc=1, device_id=to, device_id_type=MESH)

    last = s == NS - 1
    sem_s = new_sem()
    take_late = pltpu.make_async_copy(late_ref, S, sem_s)
    take_entry = pltpu.make_async_copy(entry_ref, S, sem_s)

    @pl.when(last)
    def _():
        take_entry.start()

    @pl.when(jnp.logical_not(last))
    def _():
        take_late.start()

    load_saved = load(saved_ref, SV)
    load_we1 = load(expand_early_ref, WE1)
    load_we2 = load(reduce_early_ref, WE2)
    load_gf = load(gain_first_ref, GS.at[0])
    load_sf = load(shift_first_ref, GS.at[1])
    load_w1 = load(expand_late_ref, W1.at[:, 0:HID])
    load_w2 = load(reduce_late_ref, W2.at[0:HID, :])
    load_gi = load(gain_inner_ref, GI.at[0])
    load_si = load(shift_inner_ref, SI.at[0])

    with jax.named_scope("own_stats"):
        take_late.wait()
        for q in range(Q):
            values = S[:, cols(q)].astype(F32)
            ZST[0, 0:1, cols(q)] = jnp.sum(values, axis=0, keepdims=True)
            ZST[0, 1:2, cols(q)] = jnp.sum(values * values, axis=0, keepdims=True)

    with jax.named_scope("barrier"):
        pl.semaphore_wait(barrier, len(greeted))

    with jax.named_scope("sends"):
        shift_late = [send(S.at[:, cols(q)], G.at[0, :, cols(q)], {"section": ahead}) for q in range(Q)]
        z_stats = [send(ZST.at[0], ZST.at[d], {"z": zat(d)}) for d in range(1, NZ)]

        w1_near = send(expand_late_ref, W1.at[:, HID : 2 * HID], group(1))
        w2_near = send(reduce_late_ref, W2.at[HID : 2 * HID, :], group(1))
        gains = []
        for k in (1, 2, 3):
            gains.append(send(gain_inner_ref, GI.at[k], group(k)))
            gains.append(send(shift_inner_ref, SI.at[k], group(k)))

    first_grad = s == 0
    shift_grad = []
    for p in range(PIECES):
        piece = slice(p * PR, (p + 1) * PR)
        pair = (new_sem(), new_sem())
        one = remote(exit_ref.at[piece], GR.at[piece], {"section": behind}, pair)
        two = remote(up_ref.at[piece], GR.at[piece], {"section": behind}, pair)
        shift_grad.append((one, two))

    def start_grad(p):
        one, two = shift_grad[p]
        pl.when(first_grad)(one.start)
        pl.when(jnp.logical_not(first_grad))(two.start)
        sent.append(two)

    w1_far = remote(expand_late_ref, W1.at[:, 2 * HID : 3 * HID], group(2))
    half_cols = (slice(0, CL // 2), slice(CL // 2, CL))
    w2_far = [
        remote(reduce_late_ref.at[:, at], W2.at[2 * HID : 3 * HID, at], group(2)) for at in half_cols
    ]

    def start_far(copy):
        copy.start()
        sent.append(copy)

    bulk = [functools.partial(start_grad, p) for p in range(PIECES)] + [functools.partial(start_far, w1_far)]

    def tick(n=1):
        for _ in range(n):
            if bulk:
                bulk.pop(0)()

    tick()

    with jax.named_scope("load_wait"):
        load_saved.wait()
        load_we1.wait()
        load_we2.wait()

    def early_rows(p):
        return pl.ds(pl.multiple_of(p * PR, PR), PR)

    def early_one(p, carry):
        at = early_rows(p)
        saved = SV[at, :]
        for f in range(0, FE, BLOCK):
            pre = jnp.dot(saved, WE1[:, f : f + BLOCK], preferred_element_type=F32)
            sigma = jax.nn.sigmoid(pre)
            ACT[at, f : f + BLOCK] = (pre * sigma).astype(BF16)
            DS[at, f : f + BLOCK] = sigma * (1.0 + pre * (1.0 - sigma))
        return carry

    with jax.named_scope("early_one"):
        lax.fori_loop(0, PIECES - 2, early_one, 0)

        ACC[...] = jnp.zeros(ACC.shape, F32)

    def early_two(p):
        at = slice(p * PR, (p + 1) * PR)
        with jax.named_scope("grad_wait"):
            shift_grad[p][1].wait_recv()
        with jax.named_scope("early_two"):
            grad = GR[at, :]
            saved = SV[at, :]
            result = grad.astype(F32)
            for f in range(0, FE, BLOCK):
                block = slice(f, f + BLOCK)
                back = lax.dot_general(grad, WE2[block, :], (((1,), (1,)), ((), ())), preferred_element_type=F32)
                slope = (back * DS[at, block]).astype(BF16)
                ACC[0, :, block] += lax.dot_general(saved, slope, (((0,), (0,)), ((), ())), preferred_element_type=F32)
                ACC[1, :, block] += lax.dot_general(
                    ACT[at, block], grad, (((0,), (0,)), ((), ())), preferred_element_type=F32
                )
                result += lax.dot_general(slope, WE1[:, block], (((1,), (1,)), ((), ())), preferred_element_type=F32)
            OG[at, :] = result.astype(BF16)

    hops_c, hops_a = [], []

    def forward(t, q):
        if t < H or q < Q // 2:
            hops_c.append((t, q, send(G.at[t - 1, :, cols(q)], G.at[t, :, cols(q)], {"z": zat(1)})))
        if t < H or q >= Q // 2:
            src, dst = (NZ - t + 1) % NZ, NZ - t
            hops_a.append((t, q, send(G.at[src, :, cols(q)], G.at[dst, :, cols(q)], {"z": zat(-1)})))

    def arrived(t, q):
        for hops in (hops_c, hops_a):
            for u, r, copy in hops:
                if (u, r) == (t, q):
                    copy.wait_recv()

    def shift_forward(q):
        with jax.named_scope("shift_wait"):
            shift_late[q].wait_recv()
        forward(1, q)

    shift_forward(0)
    lax.fori_loop(PIECES - 2, PIECES, early_one, 0)
    shift_forward(1)
    with jax.named_scope("zstats_wait"):
        for copy in z_stats:
            copy.wait_recv()
    total = ZST[0]
    for d in range(1, NZ):
        total = total + ZST[d]
    ZT[...] = total
    first_stats = [send(ZT, FST.at[k], {"section": ahead, **group(k)}) for k in range(4)]
    tick(2)
    for q in range(2, Q):
        shift_forward(q)

    if H > 1:
        with jax.named_scope("hop1"):
            for q in range(Q):
                arrived(1, q)
                forward(2, q)
                if q % 2:
                    tick()

    with jax.named_scope("fstats_wait"):
        for copy in first_stats:
            copy.wait_recv()
    load_gf.wait()
    load_sf.wait()
    sums = FST[0] + FST[1] + FST[2] + FST[3]
    spread, offset = affine(sums[0:1], sums[1:2], late_count, GS[0], GS[1])

    def first_of(slot):
        for q in range(Q):
            at = cols(q)
            values = G[slot, :, at].astype(F32) * spread[:, at] + offset[:, at]
            F[slot, :, at] = silu(values).astype(BF16)

    stats = [0.0, 0.0]

    def inner_of(slot):
        inner = jnp.dot(F[slot], W1[...], preferred_element_type=F32)
        INN[slot] = inner
        stats[0] += jnp.sum(inner, axis=0, keepdims=True)
        stats[1] += jnp.sum(inner * inner, axis=0, keepdims=True)

    order = [d for d in FAR_FIRST if d < NZ]
    cuts = [(0, NZ // 2), (NZ // 2, NZ)]
    factor = 1.0 / math.sqrt(e_rows * NZ * 4)

    def acc_rows(half, d):
        return pl.ds(pl.multiple_of(half * (CE // 2) + zat(d) * ZR, ZR), ZR)

    pair_sums, x_sums, z_sums, x_back, c_back, c_back_two = {}, {}, {}, {}, {}, {}
    back_c, back_a = {}, {}
    HALF = FE // 2

    def pair_send(h, k):
        lo, hi = cuts[k]
        for i in range(lo, hi):
            SD[h, i] = ACC[other_c, acc_rows(other_b if h == 0 else b, order[i]), :].astype(BF16)
        pair_sums[h, k] = send(SD.at[h, lo:hi], RD.at[h, lo:hi], group(1))

    def x_send(k):
        lo, hi = cuts[k]
        pair_sums[0, k].wait_recv()
        for i in range(lo, hi):
            SX[i] = (ACC[c, acc_rows(other_b, order[i]), :] + RD[0, i].astype(F32)).astype(BF16)
        x_sums[k] = send(SX.at[lo:hi], RX.at[lo:hi], group(2))

    def z_send(k):
        lo, hi = cuts[k]
        pair_sums[1, k].wait_recv()
        x_sums[k].wait_recv()
        for i in range(lo, hi):
            d = order[i]
            value = ACC[c, acc_rows(b, d), :] + RD[1, i].astype(F32) + RX[i].astype(F32)
            if d == 0:
                TF[...] = value
            else:
                SZ[d] = value.astype(BF16)
                z_sums[d] = send(SZ.at[d], RZ.at[d], {"z": zat(d)})

    def fin(core, half, d):
        return FIN.at[core, half, pl.ds(pl.multiple_of(zat(d) * ZR, ZR), ZR)]

    def back_to_x_and_core(d):
        piece = fin(c, b, d)
        x_back[d] = send(piece, piece, group(2))
        c_back[d] = send(piece, piece, group(1))

    def back_across(d):
        x_back[d].wait_recv()
        piece = fin(c, other_b, d)
        c_back_two[d] = send(piece, piece, group(1))

    def z_finish():
        value = TF[...]
        for d in order[::-1]:
            if d:
                z_sums[d].wait_recv()
                value = value + RZ[d].astype(F32)
        FIN[c, b, pl.ds(pl.multiple_of(z * ZR, ZR), ZR), :] = (value * factor).astype(BF16)
        z_back(1)
        back_to_x_and_core(0)

    def z_back(t):
        for back, step in ((back_c, 1), (back_a, -1)):
            piece = fin(c, b, -step * (t - 1))
            if t == H:
                piece = piece.at[:, 0:HALF] if step == 1 else piece.at[:, HALF:FE]
            back[t] = send(piece, piece, {"z": zat(step)})

    def z_forward(t):
        back_c[t].wait_recv()
        back_a[t].wait_recv()
        if t < H:
            z_back(t + 1)
            back_to_x_and_core(-t)
            back_to_x_and_core(t)
        else:
            back_to_x_and_core(H)

    def both(*slots):
        for slot in slots:
            with jax.named_scope("first"):
                first_of(slot)

    both(0)
    early_two(0)
    early = 1
    for t in range(2, H):
        with jax.named_scope(f"hop{t}"):
            for q in range(Q):
                arrived(t, q)
                forward(t + 1, q)
                if q % 2:
                    tick()
        both(t - 1, NZ - t + 1)
        early_two(early)
        early_two(early + 1)
        early += 2
    tick(len(bulk))
    with jax.named_scope("hopH"):
        for q in range(Q):
            arrived(H, q)
    both(H - 1, H + 1, H)
    for p in range(early, PIECES):
        early_two(p)
    for h in (0, 1):
        for k in (0, 1):
            pair_send(h, k)
    with jax.named_scope("X0"):
        x_send(0)
    with jax.named_scope("X1"):
        x_send(1)
    with jax.named_scope("w1_wait"):
        w1_far.wait_recv()
    w1_fwd = send(W1.at[:, 2 * HID : 3 * HID], W1.at[:, 3 * HID :], group(1))
    with jax.named_scope("w1_fwd_wait"):
        load_w1.wait()
        w1_near.wait_recv()
        w1_fwd.wait_recv()
    with jax.named_scope("inner"):
        for slot in range(NZ):
            inner_of(slot)

    IST[0, 0:1] = stats[0]
    IST[0, 1:2] = stats[1]
    inner_stats = [send(IST.at[0], IST.at[k], group(k)) for k in (1, 2, 3)]

    start_far(w2_far[0])
    start_far(w2_far[1])

    late = {}

    def second_weight(h):
        w2_far[h].wait_recv()
        late["fwd", h] = send(W2.at[2 * HID : 3 * HID, half_cols[h]], W2.at[3 * HID :, half_cols[h]], group(1))

    def second_norm():
        load_w2.wait()
        load_gi.wait()
        load_si.wait()
        w2_near.wait_recv()
        for copy in gains:
            copy.wait_recv()
        for copy in inner_stats:
            copy.wait_recv()
        spreads, offsets = [], []
        for k in range(4):
            piece = IST[0, :, k * HID : (k + 1) * HID]
            for d in (1, 2, 3):
                j = k ^ d
                piece = piece + IST[d, :, j * HID : (j + 1) * HID]
            one, two = affine(piece[0:1], piece[1:2], late_count, GI[k], SI[k])
            spreads.append(one)
            offsets.append(two)
        spread_two = jnp.concatenate(spreads, axis=1)
        offset_two = jnp.concatenate(offsets, axis=1)
        for slot in range(NZ):
            HB[slot] = silu(INN[slot] * spread_two + offset_two).astype(BF16)

    def partial_of(slot, h):
        at = half_cols[h]
        PT[slot, :, at] = jnp.dot(HB[slot], W2[:, at], preferred_element_type=F32)

    sums_c, sums_a = {}, {}

    ways = ((sums_c, SC, RC, 1), (sums_a, SA, RA, -1))

    def sum_send(way, t, q, begin):
        sums_d, S_, R_, step = way
        at = cols(q)
        value = PT[(step * (t - H)) % NZ, :, at]
        if t > begin:
            sums_d[t - 1, q].wait_recv()
            value = value + R_[t - 1, :, at].astype(F32)
        S_[t, :, at] = value.astype(BF16)
        sums_d[t, q] = send(S_.at[t, :, at], R_.at[t, :, at], {"z": zat(step)})

    def sum_begin(h):
        late["fwd", h].wait_recv()
        partial_of(H, h)
        partial_of(H - 1 if h == 0 else H + 1, h)
        for q in range(h * Q // 2, (h + 1) * Q // 2):
            sum_send(ways[h], 0, q, 0)
            sum_send(ways[1 - h], 1, q, 1)
        for slot in range(NZ):
            if slot not in (H, H - 1 if h == 0 else H + 1):
                partial_of(slot, h)

    def sum_hop(t, i):
        begin = 0 if i >= Q // 2 else 1
        sum_send(ways[0], t, (i + Q // 2) % Q, begin)
        sum_send(ways[1], t, i, begin)

    def late_final(q):
        at = cols(q)
        value = PT[0, :, at]
        if H > 1 or q < Q // 2:
            sums_c[H - 1, q].wait_recv()
            value = value + RC[H - 1, :, at].astype(F32)
        if H > 1 or q >= Q // 2:
            sums_a[H - 1, q].wait_recv()
            value = value + RA[H - 1, :, at].astype(F32)
        LO[:, at] = (G[0, :, at].astype(F32) + value).astype(BF16)

    steps = {"I": second_norm, "ZF": z_finish, "A0": functools.partial(back_across, 0)}
    for t in range(H + 1):
        for i in range(Q):
            steps[f"{t}{i}"] = functools.partial(sum_hop, t, i)
            steps[f"{i}f"] = functools.partial(late_final, i)
    for k in (0, 1):
        steps[f"W{k}"] = functools.partial(second_weight, k)
        steps[f"B{k}"] = functools.partial(sum_begin, k)
        steps[f"Z{k}"] = functools.partial(z_send, k)
    for t in range(1, H + 1):
        steps[f"R{t}"] = functools.partial(z_forward, t)
    for d in range(1, NZ):
        steps[f"A{d}"] = functools.partial(back_across, d if d <= H else d - NZ)
    for name in " ".join(PLAN).split():
        with jax.named_scope(name):
            steps[name]()
    with jax.named_scope("c_back"):
        for d in c_back:
            c_back[d].wait_recv()
            c_back_two[d].wait_recv()
    with jax.named_scope("outputs"):
        for half in (0, 1):
            at = slice(half * (CE // 2), (half + 1) * (CE // 2))
            GE[at, :] = FIN[0, half].astype(F32)
            for f in range(0, FE, BLOCK):
                OR[f + half * (CE // 2) : f + (half + 1) * (CE // 2), :] = FIN[1, half, :, f : f + BLOCK].astype(F32)

    with jax.named_scope("drain"):
        for copy in sent:
            copy.wait_send()


def place(*refs):
    sems = refs[8]
    copies = [pltpu.make_async_copy(refs[i], refs[4 + i], sems.at[i]) for i in range(4)]
    for copy in copies:
        copy.start()
    for copy in copies:
        copy.wait()


def shards(
    late_sent,
    entry_rows,
    gain_first,
    shift_first,
    expand_late,
    gain_inner,
    shift_inner,
    reduce_late,
    early_saved,
    upstream_grad,
    exit_grad,
    expand_early,
    reduce_early,
):
    rows, CL = entry_rows.shape
    e_rows, CE = exit_grad.shape
    FE = expand_early.shape[2]
    HID = expand_late.shape[2]
    NS, NZ = lax.axis_size("section"), lax.axis_size("z")
    H = NZ // 2
    VM = pltpu.VMEM
    scratch = [
        VM((rows, CL), BF16),
        VM((NZ, 2, CL), F32),
        VM((2, CL), F32),
        VM((4, 2, CL), F32),
        VM((2, 1, CL), F32),
        VM((NZ, rows, CL), BF16),
        VM((NZ, rows, CL), BF16),
        VM((CL, 4 * HID), BF16),
        VM((4 * HID, CL), BF16),
        VM((4, 1, HID), F32),
        VM((4, 1, HID), F32),
        VM((4, 2, 4 * HID), F32),
        VM((NZ, rows, 4 * HID), F32),
        VM((NZ, rows, 4 * HID), BF16),
        VM((NZ, rows, CL), F32),
        VM((H, rows, CL), BF16),
        VM((H, rows, CL), BF16),
        VM((H, rows, CL), BF16),
        VM((H, rows, CL), BF16),
        VM((e_rows, CE), BF16),
        VM((e_rows, CE), BF16),
        VM((CE, FE), BF16),
        VM((FE, CE), BF16),
        VM((e_rows, FE), BF16),
        VM((e_rows, FE), F32),
        VM((2, CE, FE), F32),
        VM((2, NZ, CE // 2 // NZ, FE), BF16),
        VM((2, NZ, CE // 2 // NZ, FE), BF16),
        VM((NZ, CE // 2 // NZ, FE), BF16),
        VM((NZ, CE // 2 // NZ, FE), BF16),
        VM((CE // 2 // NZ, FE), F32),
        VM((NZ, CE // 2 // NZ, FE), BF16),
        VM((NZ, CE // 2 // NZ, FE), BF16),
        VM((2, 2, CE // 2, FE), BF16),
        pltpu.SemaphoreType.DMA((N_SEMS,)),
    ]
    hbm = pl.BlockSpec(memory_space=pltpu.HBM)
    vmem = pl.BlockSpec(memory_space=pltpu.VMEM)
    late_out, input_grad, grad_expand, grad_reduce = pl.pallas_call(
        functools.partial(kernel, (NS, NZ)),
        out_shape=(
            VM((rows, CL), BF16),
            VM((e_rows, CE), BF16),
            VM((CE, FE), F32),
            VM((FE, CE), F32),
        ),
        in_specs=[hbm] * 13,
        out_specs=(vmem,) * 4,
        scratch_shapes=scratch,
        compiler_params=pltpu.CompilerParams(
            collective_id=0, has_side_effects=True, vmem_limit_bytes=44 * 1024 * 1024
        ),
        name="relay_step",
    )(
        *(
            pltpu.with_memory_space_constraint(x, pltpu.HBM)
            for x in (
                late_sent[0],
                entry_rows,
                gain_first,
                shift_first,
                expand_late[0],
                gain_inner,
                shift_inner,
                reduce_late[0],
                early_saved[0],
                upstream_grad[0],
                exit_grad,
                expand_early[0],
                reduce_early[0],
            )
        )
    )
    results = (late_out, input_grad, grad_expand, grad_reduce)
    results = pl.pallas_call(
        place,
        out_shape=tuple(jax.ShapeDtypeStruct(x.shape, x.dtype) for x in results),
        in_specs=[vmem] * 4,
        out_specs=(pl.BlockSpec(memory_space=pl.ANY),) * 4,
        scratch_shapes=[pltpu.SemaphoreType.DMA((4,))],
        compiler_params=pltpu.CompilerParams(vmem_limit_bytes=4 * 1024 * 1024),
        name="place",
    )(*results)
    return tuple(x[None] for x in results)


def solution(mesh):
    sections, devices = mesh.devices.shape
    split = Mesh(mesh.devices.reshape(sections, 2, devices // 4, 2), ("section", *DEV))
    return jax.shard_map(
        shards,
        mesh=split,
        in_specs=(
            P("section", DEV, None),
            P(DEV, None),
            P("section", None),
            P("section", None),
            P("section", None, DEV),
            P("section", DEV),
            P("section", DEV),
            P("section", DEV, None),
            P("section", DEV, None),
            P("section", DEV, None),
            P(DEV, None),
            P("section", None, None),
            P("section", None, None),
        ),
        out_specs=(
            P("section", DEV, None),
            P("section", DEV, None),
            P("section", None, None),
            P("section", None, None),
        ),
        check_vma=False,
    )
```

```python
import functools
import math

import jax
import jax.numpy as jnp
from jax import lax
from jax.experimental import pallas as pl
from jax.experimental.pallas import tpu as pltpu
from jax.sharding import Mesh
from jax.sharding import PartitionSpec as P

DEV = ("b", "z", "c")
MESH = pl.DeviceIdType.MESH
F32 = jnp.float32
BF16 = jnp.bfloat16
EPS = 1e-05
Q = 4
PIECES = 7
BLOCK = 256
N_SEMS = 400
PLAN = (
    "Z0 Z1 I W0",
    "B0 ZF W1 B1",
    "12 13 R1 R2",
    "A0 20 21 22",
    "23 A7 A1 30",
    "R3 R4 A6 A2",
    "31 32 33 A5",
    "A3 0f 1f A4",
    "2f 3f",
)
FAR_FIRST = (4, 3, 5, 2, 6, 1, 7, 0)


def silu(v):
    return v * jax.nn.sigmoid(v)


def affine(sums, squares, count, gain, shift):
    average = sums / count
    second = squares / count
    spread = gain * lax.rsqrt(second - average * average + EPS)
    return spread, shift - average * spread


def kernel(
    sizes,
    late_ref,
    entry_ref,
    gain_first_ref,
    shift_first_ref,
    expand_late_ref,
    gain_inner_ref,
    shift_inner_ref,
    reduce_late_ref,
    saved_ref,
    up_ref,
    exit_ref,
    expand_early_ref,
    reduce_early_ref,
    LO,
    OG,
    GE,
    OR,
    S,
    ZST,
    ZT,
    FST,
    GS,
    G,
    F,
    W1,
    W2,
    GI,
    SI,
    IST,
    INN,
    HB,
    PT,
    SC,
    SA,
    RC,
    RA,
    SV,
    GR,
    WE1,
    WE2,
    ACT,
    DS,
    ACC,
    SD,
    RD,
    SX,
    RX,
    TF,
    SZ,
    RZ,
    FIN,
    sems,
):
    NS, NZ = sizes
    H = NZ // 2
    assert H == 4
    rows, CL = S.shape
    CQ = CL // Q
    HID = expand_late_ref.shape[1]
    e_rows, CE = SV.shape
    FE = WE1.shape[1]
    PR = e_rows // PIECES
    ZR = CE // 2 // NZ
    late_count = rows * NZ * 4

    s = lax.axis_index("section")
    b = lax.axis_index("b")
    z = lax.axis_index("z")
    c = lax.axis_index("c")
    ahead = lax.rem(s + 1, NS)
    behind = lax.rem(s + NS - 1, NS)
    other_b = 1 - b
    other_c = 1 - c

    def zat(d):
        return lax.rem(z + d + NZ, NZ)

    def group(k):
        where = {}
        if k & 2:
            where["b"] = other_b
        if k & 1:
            where["c"] = other_c
        return where

    used = [0]
    sent = []

    def new_sem():
        used[0] += 1
        return sems.at[used[0] - 1]

    def remote(src, dst, to, pair=None):
        pair = pair or (new_sem(), new_sem())
        return pltpu.make_async_remote_copy(
            src_ref=src, dst_ref=dst, send_sem=pair[0], recv_sem=pair[1], device_id=to, device_id_type=MESH
        )

    def send(src, dst, to):
        copy = remote(src, dst, to)
        copy.start()
        sent.append(copy)
        return copy

    def load(src, dst):
        copy = pltpu.make_async_copy(src, dst, new_sem())
        copy.start()
        return copy

    def cols(q):
        return slice(q * CQ, (q + 1) * CQ)

    barrier = pltpu.get_barrier_semaphore()
    greeted = [{"z": zat(d)} for d in range(1, NZ)] + [group(k) for k in (1, 2, 3)]
    greeted += [{"section": ahead, **group(k)} for k in range(4)]
    greeted += [{"section": behind, **group(k)} for k in range(4)]
    with jax.named_scope("greet"):
        for to in greeted:
            pl.semaphore_signal(barrier, inc=1, device_id=to, device_id_type=MESH)

    last = s == NS - 1
    sem_s = new_sem()
    take_late = pltpu.make_async_copy(late_ref, S, sem_s)
    take_entry = pltpu.make_async_copy(entry_ref, S, sem_s)

    @pl.when(last)
    def _():
        take_entry.start()

    @pl.when(jnp.logical_not(last))
    def _():
        take_late.start()

    load_saved = load(saved_ref, SV)
    load_we1 = load(expand_early_ref, WE1)
    load_we2 = load(reduce_early_ref, WE2)
    load_gf = load(gain_first_ref, GS.at[0])
    load_sf = load(shift_first_ref, GS.at[1])
    load_w1 = load(expand_late_ref, W1.at[:, 0:HID])
    load_w2 = load(reduce_late_ref, W2.at[0:HID, :])
    load_gi = load(gain_inner_ref, GI.at[0])
    load_si = load(shift_inner_ref, SI.at[0])

    with jax.named_scope("own_stats"):
        take_late.wait()
        for q in range(Q):
            values = S[:, cols(q)].astype(F32)
            ZST[0, 0:1, cols(q)] = jnp.sum(values, axis=0, keepdims=True)
            ZST[0, 1:2, cols(q)] = jnp.sum(values * values, axis=0, keepdims=True)

    with jax.named_scope("barrier"):
        pl.semaphore_wait(barrier, len(greeted))

    with jax.named_scope("sends"):
        shift_late = [send(S.at[:, cols(q)], G.at[0, :, cols(q)], {"section": ahead}) for q in range(Q)]
        z_stats = [send(ZST.at[0], ZST.at[d], {"z": zat(d)}) for d in range(1, NZ)]

        w1_near = send(expand_late_ref, W1.at[:, HID : 2 * HID], group(1))
        w2_near = send(reduce_late_ref, W2.at[HID : 2 * HID, :], group(1))
        gains = []
        for k in (1, 2, 3):
            gains.append(send(gain_inner_ref, GI.at[k], group(k)))
            gains.append(send(shift_inner_ref, SI.at[k], group(k)))

    first_grad = s == 0
    shift_grad = []
    for p in range(PIECES):
        piece = slice(p * PR, (p + 1) * PR)
        pair = (new_sem(), new_sem())
        one = remote(exit_ref.at[piece], GR.at[piece], {"section": behind}, pair)
        two = remote(up_ref.at[piece], GR.at[piece], {"section": behind}, pair)
        shift_grad.append((one, two))

    def start_grad(p):
        one, two = shift_grad[p]
        pl.when(first_grad)(one.start)
        pl.when(jnp.logical_not(first_grad))(two.start)
        sent.append(two)

    w1_far = remote(expand_late_ref, W1.at[:, 2 * HID : 3 * HID], group(2))
    half_cols = (slice(0, CL // 2), slice(CL // 2, CL))
    w2_far = [
        remote(reduce_late_ref.at[:, at], W2.at[2 * HID : 3 * HID, at], group(2)) for at in half_cols
    ]

    def start_far(copy):
        copy.start()
        sent.append(copy)

    bulk = [functools.partial(start_grad, p) for p in range(PIECES)] + [functools.partial(start_far, w1_far)]

    def tick(n=1):
        for _ in range(n):
            if bulk:
                bulk.pop(0)()

    tick()

    with jax.named_scope("load_wait"):
        load_saved.wait()
        load_we1.wait()
        load_we2.wait()

    def early_rows(p):
        return pl.ds(pl.multiple_of(p * PR, PR), PR)

    def early_one(p, carry):
        at = early_rows(p)
        saved = SV[at, :]
        for f in range(0, FE, BLOCK):
            pre = jnp.dot(saved, WE1[:, f : f + BLOCK], preferred_element_type=F32)
            sigma = jax.nn.sigmoid(pre)
            ACT[at, f : f + BLOCK] = (pre * sigma).astype(BF16)
            DS[at, f : f + BLOCK] = sigma * (1.0 + pre * (1.0 - sigma))
        return carry

    with jax.named_scope("early_one"):
        lax.fori_loop(0, PIECES - 2, early_one, 0)

        ACC[...] = jnp.zeros(ACC.shape, F32)

    def early_two(p):
        at = slice(p * PR, (p + 1) * PR)
        with jax.named_scope("grad_wait"):
            shift_grad[p][1].wait_recv()
        with jax.named_scope("early_two"):
            grad = GR[at, :]
            saved = SV[at, :]
            result = grad.astype(F32)
            for f in range(0, FE, BLOCK):
                block = slice(f, f + BLOCK)
                back = lax.dot_general(grad, WE2[block, :], (((1,), (1,)), ((), ())), preferred_element_type=F32)
                slope = (back * DS[at, block]).astype(BF16)
                ACC[0, :, block] += lax.dot_general(saved, slope, (((0,), (0,)), ((), ())), preferred_element_type=F32)
                ACC[1, :, block] += lax.dot_general(
                    ACT[at, block], grad, (((0,), (0,)), ((), ())), preferred_element_type=F32
                )
                result += lax.dot_general(slope, WE1[:, block], (((1,), (1,)), ((), ())), preferred_element_type=F32)
            OG[at, :] = result.astype(BF16)

    hops_c, hops_a = [], []

    def forward(t, q):
        if t < H or q < Q // 2:
            hops_c.append((t, q, send(G.at[t - 1, :, cols(q)], G.at[t, :, cols(q)], {"z": zat(1)})))
        if t < H or q >= Q // 2:
            src, dst = (NZ - t + 1) % NZ, NZ - t
            hops_a.append((t, q, send(G.at[src, :, cols(q)], G.at[dst, :, cols(q)], {"z": zat(-1)})))

    def arrived(t, q):
        for hops in (hops_c, hops_a):
            for u, r, copy in hops:
                if (u, r) == (t, q):
                    copy.wait_recv()

    def shift_forward(q):
        with jax.named_scope("shift_wait"):
            shift_late[q].wait_recv()
        forward(1, q)

    shift_forward(0)
    lax.fori_loop(PIECES - 2, PIECES, early_one, 0)
    shift_forward(1)
    with jax.named_scope("zstats_wait"):
        for copy in z_stats:
            copy.wait_recv()
    total = ZST[0]
    for d in range(1, NZ):
        total = total + ZST[d]
    ZT[...] = total
    first_stats = [send(ZT, FST.at[k], {"section": ahead, **group(k)}) for k in range(4)]
    tick(2)
    for q in range(2, Q):
        shift_forward(q)

    if H > 1:
        with jax.named_scope("hop1"):
            for q in range(Q):
                arrived(1, q)
                forward(2, q)
                if q % 2:
                    tick()

    with jax.named_scope("fstats_wait"):
        for copy in first_stats:
            copy.wait_recv()
    load_gf.wait()
    load_sf.wait()
    sums = FST[0] + FST[1] + FST[2] + FST[3]
    spread, offset = affine(sums[0:1], sums[1:2], late_count, GS[0], GS[1])

    def first_of(slot):
        for q in range(Q):
            at = cols(q)
            values = G[slot, :, at].astype(F32) * spread[:, at] + offset[:, at]
            F[slot, :, at] = silu(values).astype(BF16)

    stats = [0.0, 0.0]

    def inner_of(slot):
        inner = jnp.dot(F[slot], W1[...], preferred_element_type=F32)
        INN[slot] = inner
        stats[0] += jnp.sum(inner, axis=0, keepdims=True)
        stats[1] += jnp.sum(inner * inner, axis=0, keepdims=True)

    order = [d for d in FAR_FIRST if d < NZ]
    cuts = [(0, NZ // 2), (NZ // 2, NZ)]
    factor = 1.0 / math.sqrt(e_rows * NZ * 4)

    def acc_rows(half, d):
        return pl.ds(pl.multiple_of(half * (CE // 2) + zat(d) * ZR, ZR), ZR)

    pair_sums, x_sums, z_sums, x_back, c_back, c_back_two = {}, {}, {}, {}, {}, {}
    back = {}
    HALF = FE // 2

    def pair_send(h, k):
        lo, hi = cuts[k]
        for i in range(lo, hi):
            SD[h, i] = ACC[other_c, acc_rows(other_b if h == 0 else b, order[i]), :].astype(BF16)
        pair_sums[h, k] = send(SD.at[h, lo:hi], RD.at[h, lo:hi], group(1))

    def x_send(k):
        lo, hi = cuts[k]
        pair_sums[0, k].wait_recv()
        for i in range(lo, hi):
            SX[i] = (ACC[c, acc_rows(other_b, order[i]), :] + RD[0, i].astype(F32)).astype(BF16)
        x_sums[k] = send(SX.at[lo:hi], RX.at[lo:hi], group(2))

    def z_send(k):
        lo, hi = cuts[k]
        pair_sums[1, k].wait_recv()
        x_sums[k].wait_recv()
        for i in range(lo, hi):
            d = order[i]
            value = ACC[c, acc_rows(b, d), :] + RD[1, i].astype(F32) + RX[i].astype(F32)
            if d == 0:
                TF[...] = value
            else:
                SZ[d] = value.astype(BF16)
                z_sums[d] = send(SZ.at[d], RZ.at[d], {"z": zat(d)})

    def fin(core, half, d):
        return FIN.at[core, half, pl.ds(pl.multiple_of(zat(d) * ZR, ZR), ZR)]

    def back_to_x_and_core(d):
        piece = fin(c, b, d)
        x_back[d] = send(piece, piece, group(2))
        c_back[d] = send(piece, piece, group(1))

    def back_across(d):
        x_back[d].wait_recv()
        piece = fin(c, other_b, d)
        c_back_two[d] = send(piece, piece, group(1))

    def z_finish():
        value = TF[...]
        for d in order[::-1]:
            if d:
                z_sums[d].wait_recv()
                value = value + RZ[d].astype(F32)
        FIN[c, b, pl.ds(pl.multiple_of(z * ZR, ZR), ZR), :] = (value * factor).astype(BF16)
        for by in (1, -1, 2, -2):
            z_back(by, 0, by)
        back_to_x_and_core(0)

    def z_back(key, d, by, at=slice(None)):
        piece = fin(c, b, d).at[:, at]
        back[key] = send(piece, piece, {"z": zat(by)})

    def z_forward(t):
        if t < H:
            back[t].wait_recv()
            back[-t].wait_recv()
            if t == 2:
                z_back(3, -2, 1)
                z_back(-3, 2, -1)
                z_back("c", -2, 2, slice(0, HALF))
                z_back("a", 2, -2, slice(HALF, FE))
            back_to_x_and_core(-t)
            back_to_x_and_core(t)
        else:
            back["c"].wait_recv()
            back["a"].wait_recv()
            back_to_x_and_core(H)

    def both(*slots):
        for slot in slots:
            with jax.named_scope("first"):
                first_of(slot)

    both(0)
    early_two(0)
    early = 1
    for t in range(2, H):
        with jax.named_scope(f"hop{t}"):
            for q in range(Q):
                arrived(t, q)
                forward(t + 1, q)
                if q % 2:
                    tick()
        both(t - 1, NZ - t + 1)
        early_two(early)
        early_two(early + 1)
        early += 2
    tick(len(bulk))
    with jax.named_scope("hopH"):
        for q in range(Q):
            arrived(H, q)
    both(H - 1, H + 1, H)
    for p in range(early, PIECES):
        early_two(p)
    for h in (0, 1):
        for k in (0, 1):
            pair_send(h, k)
    with jax.named_scope("X0"):
        x_send(0)
    with jax.named_scope("X1"):
        x_send(1)
    with jax.named_scope("w1_wait"):
        w1_far.wait_recv()
    w1_fwd = send(W1.at[:, 2 * HID : 3 * HID], W1.at[:, 3 * HID :], group(1))
    with jax.named_scope("w1_fwd_wait"):
        load_w1.wait()
        w1_near.wait_recv()
        w1_fwd.wait_recv()
    with jax.named_scope("inner"):
        for slot in range(NZ):
            inner_of(slot)

    IST[0, 0:1] = stats[0]
    IST[0, 1:2] = stats[1]
    inner_stats = [send(IST.at[0], IST.at[k], group(k)) for k in (1, 2, 3)]

    start_far(w2_far[0])
    start_far(w2_far[1])

    late = {}

    def second_weight(h):
        w2_far[h].wait_recv()
        late["fwd", h] = send(W2.at[2 * HID : 3 * HID, half_cols[h]], W2.at[3 * HID :, half_cols[h]], group(1))

    def second_norm():
        load_w2.wait()
        load_gi.wait()
        load_si.wait()
        w2_near.wait_recv()
        for copy in gains:
            copy.wait_recv()
        for copy in inner_stats:
            copy.wait_recv()
        spreads, offsets = [], []
        for k in range(4):
            piece = IST[0, :, k * HID : (k + 1) * HID]
            for d in (1, 2, 3):
                j = k ^ d
                piece = piece + IST[d, :, j * HID : (j + 1) * HID]
            one, two = affine(piece[0:1], piece[1:2], late_count, GI[k], SI[k])
            spreads.append(one)
            offsets.append(two)
        spread_two = jnp.concatenate(spreads, axis=1)
        offset_two = jnp.concatenate(offsets, axis=1)
        for slot in range(NZ):
            HB[slot] = silu(INN[slot] * spread_two + offset_two).astype(BF16)

    def partial_of(slot, h):
        at = half_cols[h]
        PT[slot, :, at] = jnp.dot(HB[slot], W2[:, at], preferred_element_type=F32)

    sums_c, sums_a = {}, {}

    ways = ((sums_c, SC, RC, 1), (sums_a, SA, RA, -1))

    def sum_send(way, t, q, begin):
        sums_d, S_, R_, step = way
        at = cols(q)
        value = PT[(step * (t - H)) % NZ, :, at]
        if t > begin:
            sums_d[t - 1, q].wait_recv()
            value = value + R_[t - 1, :, at].astype(F32)
        S_[t, :, at] = value.astype(BF16)
        sums_d[t, q] = send(S_.at[t, :, at], R_.at[t, :, at], {"z": zat(step)})

    def sum_begin(h):
        late["fwd", h].wait_recv()
        partial_of(H, h)
        partial_of(H - 1 if h == 0 else H + 1, h)
        for q in range(h * Q // 2, (h + 1) * Q // 2):
            sum_send(ways[h], 0, q, 0)
            sum_send(ways[1 - h], 1, q, 1)
        for slot in range(NZ):
            if slot not in (H, H - 1 if h == 0 else H + 1):
                partial_of(slot, h)

    def sum_hop(t, i):
        begin = 0 if i >= Q // 2 else 1
        sum_send(ways[0], t, (i + Q // 2) % Q, begin)
        sum_send(ways[1], t, i, begin)

    def late_final(q):
        at = cols(q)
        value = PT[0, :, at]
        if H > 1 or q < Q // 2:
            sums_c[H - 1, q].wait_recv()
            value = value + RC[H - 1, :, at].astype(F32)
        if H > 1 or q >= Q // 2:
            sums_a[H - 1, q].wait_recv()
            value = value + RA[H - 1, :, at].astype(F32)
        LO[:, at] = (G[0, :, at].astype(F32) + value).astype(BF16)

    steps = {"I": second_norm, "ZF": z_finish, "A0": functools.partial(back_across, 0)}
    for t in range(H + 1):
        for i in range(Q):
            steps[f"{t}{i}"] = functools.partial(sum_hop, t, i)
            steps[f"{i}f"] = functools.partial(late_final, i)
    for k in (0, 1):
        steps[f"W{k}"] = functools.partial(second_weight, k)
        steps[f"B{k}"] = functools.partial(sum_begin, k)
        steps[f"Z{k}"] = functools.partial(z_send, k)
    for t in range(1, H + 1):
        steps[f"R{t}"] = functools.partial(z_forward, t)
    for d in range(1, NZ):
        steps[f"A{d}"] = functools.partial(back_across, d if d <= H else d - NZ)
    for name in " ".join(PLAN).split():
        with jax.named_scope(name):
            steps[name]()
    with jax.named_scope("c_back"):
        for d in c_back:
            c_back[d].wait_recv()
            c_back_two[d].wait_recv()
    with jax.named_scope("outputs"):
        for half in (0, 1):
            at = slice(half * (CE // 2), (half + 1) * (CE // 2))
            GE[at, :] = FIN[0, half].astype(F32)
            for f in range(0, FE, BLOCK):
                OR[f + half * (CE // 2) : f + (half + 1) * (CE // 2), :] = FIN[1, half, :, f : f + BLOCK].astype(F32)

    with jax.named_scope("drain"):
        for copy in sent:
            copy.wait_send()


def place(*refs):
    sems = refs[8]
    copies = [pltpu.make_async_copy(refs[i], refs[4 + i], sems.at[i]) for i in range(4)]
    for copy in copies:
        copy.start()
    for copy in copies:
        copy.wait()


def shards(
    late_sent,
    entry_rows,
    gain_first,
    shift_first,
    expand_late,
    gain_inner,
    shift_inner,
    reduce_late,
    early_saved,
    upstream_grad,
    exit_grad,
    expand_early,
    reduce_early,
):
    rows, CL = entry_rows.shape
    e_rows, CE = exit_grad.shape
    FE = expand_early.shape[2]
    HID = expand_late.shape[2]
    NS, NZ = lax.axis_size("section"), lax.axis_size("z")
    H = NZ // 2
    VM = pltpu.VMEM
    scratch = [
        VM((rows, CL), BF16),
        VM((NZ, 2, CL), F32),
        VM((2, CL), F32),
        VM((4, 2, CL), F32),
        VM((2, 1, CL), F32),
        VM((NZ, rows, CL), BF16),
        VM((NZ, rows, CL), BF16),
        VM((CL, 4 * HID), BF16),
        VM((4 * HID, CL), BF16),
        VM((4, 1, HID), F32),
        VM((4, 1, HID), F32),
        VM((4, 2, 4 * HID), F32),
        VM((NZ, rows, 4 * HID), F32),
        VM((NZ, rows, 4 * HID), BF16),
        VM((NZ, rows, CL), F32),
        VM((H, rows, CL), BF16),
        VM((H, rows, CL), BF16),
        VM((H, rows, CL), BF16),
        VM((H, rows, CL), BF16),
        VM((e_rows, CE), BF16),
        VM((e_rows, CE), BF16),
        VM((CE, FE), BF16),
        VM((FE, CE), BF16),
        VM((e_rows, FE), BF16),
        VM((e_rows, FE), F32),
        VM((2, CE, FE), F32),
        VM((2, NZ, CE // 2 // NZ, FE), BF16),
        VM((2, NZ, CE // 2 // NZ, FE), BF16),
        VM((NZ, CE // 2 // NZ, FE), BF16),
        VM((NZ, CE // 2 // NZ, FE), BF16),
        VM((CE // 2 // NZ, FE), F32),
        VM((NZ, CE // 2 // NZ, FE), BF16),
        VM((NZ, CE // 2 // NZ, FE), BF16),
        VM((2, 2, CE // 2, FE), BF16),
        pltpu.SemaphoreType.DMA((N_SEMS,)),
    ]
    hbm = pl.BlockSpec(memory_space=pltpu.HBM)
    vmem = pl.BlockSpec(memory_space=pltpu.VMEM)
    late_out, input_grad, grad_expand, grad_reduce = pl.pallas_call(
        functools.partial(kernel, (NS, NZ)),
        out_shape=(
            VM((rows, CL), BF16),
            VM((e_rows, CE), BF16),
            VM((CE, FE), F32),
            VM((FE, CE), F32),
        ),
        in_specs=[hbm] * 13,
        out_specs=(vmem,) * 4,
        scratch_shapes=scratch,
        compiler_params=pltpu.CompilerParams(
            collective_id=0, has_side_effects=True, vmem_limit_bytes=44 * 1024 * 1024
        ),
        name="relay_step",
    )(
        *(
            pltpu.with_memory_space_constraint(x, pltpu.HBM)
            for x in (
                late_sent[0],
                entry_rows,
                gain_first,
                shift_first,
                expand_late[0],
                gain_inner,
                shift_inner,
                reduce_late[0],
                early_saved[0],
                upstream_grad[0],
                exit_grad,
                expand_early[0],
                reduce_early[0],
            )
        )
    )
    results = (late_out, input_grad, grad_expand, grad_reduce)
    results = pl.pallas_call(
        place,
        out_shape=tuple(jax.ShapeDtypeStruct(x.shape, x.dtype) for x in results),
        in_specs=[vmem] * 4,
        out_specs=(pl.BlockSpec(memory_space=pl.ANY),) * 4,
        scratch_shapes=[pltpu.SemaphoreType.DMA((4,))],
        compiler_params=pltpu.CompilerParams(vmem_limit_bytes=4 * 1024 * 1024),
        name="place",
    )(*results)
    return tuple(x[None] for x in results)


def solution(mesh):
    sections, devices = mesh.devices.shape
    split = Mesh(mesh.devices.reshape(sections, 2, devices // 4, 2), ("section", *DEV))
    return jax.shard_map(
        shards,
        mesh=split,
        in_specs=(
            P("section", DEV, None),
            P(DEV, None),
            P("section", None),
            P("section", None),
            P("section", None, DEV),
            P("section", DEV),
            P("section", DEV),
            P("section", DEV, None),
            P("section", DEV, None),
            P("section", DEV, None),
            P(DEV, None),
            P("section", None, None),
            P("section", None, None),
        ),
        out_specs=(
            P("section", DEV, None),
            P("section", DEV, None),
            P("section", None, None),
            P("section", None, None),
        ),
        check_vma=False,
    )
```
